32 devices in a mesh: worker: 8 (over y, x, core), mp: 4 (over z).
Axes of the slice: x: 2, y: 2, z: 4, core: 2. Of those that a mesh axis runs over, the one named last changes fastest.
Arguments:
- gradients: float32 [8, 2097152], P('worker', 'mp'), may hold values from -100 to 100
- neighbours: int32 [8, 3], replicated, may hold values from 0 to 7, as said below
- winner: int32 [1], replicated, may hold values from 0 to 7
Outputs:
- scores: float32 [8], replicated
- aggregate: float32 [2097152], P(('mp', 'worker'))
The draws below stay inside these ranges and needn't reach their ends.
Inputs may be any that keep to these rules, and one draw needn't show every extreme that they name: `neighbours`: row i lists 3 different workers, none of them equal to i.
All inputs are finite; a program needn't handle non-finite values.
Results may differ from the reference program's by a relative error of at most 0.0003.
Values may be sent and summed in bfloat16 or wider, within the bound.
A program may use at most 64 MiB of HBM per device.

```python
import math
import jax
import jax.numpy as jnp
from jax import lax

FAULTY = 3
WORKERS = 8
NBR = 3
PARAMS = 2097152


def draw_gradients(key, part):
    keys = jax.random.split(jax.random.fold_in(key, 11), 10)
    noise = jnp.clip(jax.random.normal(keys[0], (WORKERS, PARAMS), jnp.float32), -6.0, 6.0)
    position = jnp.arange(PARAMS, dtype=jnp.float32) / jnp.float32(PARAMS)
    scales = jnp.exp(jax.random.uniform(keys[1], (WORKERS, 1), jnp.float32, math.log(0.5), math.log(2.0)))
    column = 0.5 * jnp.exp(math.log(3.0) * position)[None, :]
    values = scales * column * noise
    loadings = jax.random.uniform(keys[8], (WORKERS, 4), jnp.float32, -1.0, 1.0)
    shared = jnp.clip(jax.random.normal(keys[9], (4, PARAMS), jnp.float32), -6.0, 6.0)
    for factor in range(4):
        values = values + column * loadings[:, factor:factor + 1] * shared[factor][None, :]
    ranking = jax.random.permutation(keys[4], WORKERS)
    faulty = (ranking < FAULTY).astype(jnp.float32)[:, None]
    sparse = (jax.random.uniform(keys[5], (WORKERS, PARAMS), jnp.float32) < 1.0 / 4096.0).astype(jnp.float32)
    size = jax.random.uniform(keys[6], (WORKERS, PARAMS), jnp.float32, 20.0, 40.0)
    sign = jnp.where(jax.random.uniform(keys[7], (WORKERS, PARAMS), jnp.float32) < 0.5, -1.0, 1.0)
    values = values + faulty * sparse * sign * size * column
    return jnp.clip(values, -100.0, 100.0).astype(jnp.float32)


def draw_neighbours(key, part):
    keys = jax.random.split(jax.random.fold_in(key, 23), WORKERS)
    orders = jax.vmap(lambda single: jax.random.permutation(single, WORKERS - 1))(keys)[:, :NBR]
    orders = orders.astype(jnp.int32)
    own_index = jnp.arange(WORKERS, dtype=jnp.int32)[:, None]
    return (orders + (orders >= own_index).astype(jnp.int32)).astype(jnp.int32)


def setup_inputs(seed: int = 0) -> dict:
    streams_of = jax.random.split(jax.random.key(seed), 4)
    return {
        "gradients": draw_gradients(jax.random.fold_in(streams_of[3], 71), 0),
        "neighbours": draw_neighbours(jax.random.fold_in(streams_of[3], 71), 0),
        "winner": jax.random.randint(streams_of[2], (1,), 0, WORKERS).astype(jnp.int32),
    }


def reference(gradients, neighbours, winner):
    rounded = gradients.astype(jnp.bfloat16)
    gram_matrix = jnp.dot(rounded, rounded.T, preferred_element_type=jnp.float32)
    squares = jnp.diagonal(gram_matrix)
    distance = squares[:, None] + squares[None, :] - 2.0 * gram_matrix
    chosen = jnp.take_along_axis(distance, neighbours, axis=1)
    scores = jnp.sum(chosen, axis=1) / jnp.float32(NBR * PARAMS)
    aggregate = lax.dynamic_index_in_dim(gradients, winner[0], 0, keepdims=False)
    return (scores, aggregate)
```

```python
import functools

import jax
import jax.numpy as jnp
from jax import lax
from jax.experimental import pallas as pl
from jax.experimental.pallas import tpu as pltpu
from jax.sharding import PartitionSpec as P

MESH = pl.DeviceIdType.MESH
LANES = 128
CHUNKS = 4


def flip(index, offset, size):
    result, bit = 0, 1
    while bit < size:
        digit = (index // bit) % 2
        if (offset // bit) % 2:
            digit = 1 - digit
        result = result + digit * bit
        bit *= 2
    return result


def kernel(
    workers,
    planes,
    total_entries,
    nb_hbm,
    win_ref,
    g_ref,
    scores_ref,
    out_ref,
    nb_ref,
    stage,
    rounded,
    recv,
    rest,
    rest_in,
    rest_recv,
    relay,
    dist,
    part,
    score_rows,
    small_sem,
    load_sem,
    gsend,
    grecv,
    osend,
    orecv,
    ysend,
    yrecv,
    rsend,
    rrecv,
    ssend,
    srecv,
):
    me = lax.axis_index("worker")
    plane = lax.axis_index("mp")
    core = me % 2
    chip = me // 2
    chips = workers // 2
    rows = stage.shape[1]
    span = rows // CHUNKS
    order = sorted(range(2, workers), key=lambda o: (-bin(o // 2).count("1"), o // 2, o % 2)) + [1, 0]
    peer = [flip(me, o, workers) for o in range(workers)]

    barrier = pltpu.get_barrier_semaphore()
    for o in range(1, workers):
        pl.semaphore_signal(barrier, inc=1, device_id={"worker": peer[o]}, device_id_type=MESH)
    for z in range(1, planes):
        pl.semaphore_signal(
            barrier, inc=1, device_id={"mp": (plane + z) % planes}, device_id_type=MESH
        )

    def load(o, c):
        first = pl.multiple_of(peer[o] * rows + c * span, span)
        return pltpu.make_async_copy(
            g_ref.at[pl.ds(first, span), :],
            stage.at[o, pl.ds(c * span, span), :],
            load_sem.at[o, c],
        )

    for c in range(CHUNKS):
        for o in order:
            load(o, c).start()
    lists = pltpu.make_async_copy(nb_hbm, nb_ref, small_sem)
    lists.start()

    def gram_copy(o, c, slot):
        at = pl.ds(c * span, span)
        return pltpu.make_async_remote_copy(
            src_ref=rounded.at[o, at, :],
            dst_ref=recv.at[slot, at, :],
            send_sem=gsend.at[o, c],
            recv_sem=grecv.at[o, c],
            device_id={"worker": peer[o]},
            device_id_type=MESH,
        )

    keep = jnp.where(win_ref[0] == me, 1.0, 0.0).astype(jnp.float32)

    def convert(o, c):
        at = pl.ds(c * span, span)
        x = stage[o, at, :]
        hi = x.astype(jnp.bfloat16)
        if o == 0:
            recv[me, at, :] = hi
        else:
            rounded[o, at, :] = hi
        low = ((x - hi.astype(jnp.float32)) * keep).astype(jnp.bfloat16)
        rest[peer[o] % 2, peer[o] // 2, at, :] = low

    def swap(ox):
        there = flip(chip, ox, chips)
        return pltpu.make_async_remote_copy(
            src_ref=rest.at[1 - core, there],
            dst_ref=rest_in.at[there],
            send_sem=osend.at[ox],
            recv_sem=orecv.at[ox],
            device_id={"worker": peer[1]},
            device_id_type=MESH,
        )

    def add_to_rest(there, at, other):
        rest_in[there, at, :] = rest_in[there, at, :] + other

    def combine(ox):
        there = flip(chip, ox, chips)
        swap(ox).wait_recv()
        for c in range(CHUNKS):
            at = pl.ds(c * span, span)
            add_to_rest(there, at, rest[core, there, at, :])

    split = chips == 4
    half = rows // 2

    def relay_copy(ox):
        return pltpu.make_async_remote_copy(
            src_ref=rest_in.at[flip(chip, 3, chips), pl.ds((ox - 1) * half, half), :],
            dst_ref=relay.at[ox - 1],
            send_sem=ysend.at[ox - 1],
            recv_sem=yrecv.at[ox - 1],
            device_id={"worker": peer[2 * ox]},
            device_id_type=MESH,
        )

    def rest_copy(ox, n):
        at = pl.ds(n * half, half)
        return pltpu.make_async_remote_copy(
            src_ref=rest_in.at[flip(chip, ox, chips), at, :],
            dst_ref=rest_recv.at[ox, at, :],
            send_sem=rsend.at[ox, n],
            recv_sem=rrecv.at[ox, n],
            device_id={"worker": peer[2 * ox]},
            device_id_type=MESH,
        )

    rest_order = sorted(range(1, chips), key=lambda ox: bin(ox).count("1"))
    if split:
        rest_order = [1, 2]

    first = True
    for c in range(CHUNKS):
        for o in order:
            load(o, c).wait()
            convert(o, c)
            if first:
                pl.semaphore_wait(barrier, workers - 1 + planes - 1)
                first = False
            if o:
                gram_copy(o, c, me).start()
    for ox in range(chips):
        swap(ox).start()

    pairs = [(i, k) for i in range(workers) for k in range(i, workers)]

    def gram(first, accs):
        def one(step, accs):
            at = pl.ds(pl.multiple_of(first + step * 16, 16), 16)
            xs = [recv[i, at, :].astype(jnp.float32) for i in range(workers)]
            lo = [x[:8] for x in xs]
            hi = [x[8:] for x in xs]
            return tuple(
                a + (lo[i] * lo[k] + hi[i] * hi[k]) for a, (i, k) in zip(accs, pairs)
            )

        return lax.fori_loop(0, span // 16, one, accs)

    accs = tuple(jnp.zeros((8, LANES), jnp.float32) for _ in pairs)
    for c in range(CHUNKS):
        if c == CHUNKS - 1:
            for ox in reversed(range(chips)):
                combine(ox)
            if split:
                relay_copy(1).start()
                relay_copy(2).start()
        for o in order[:-1]:
            gram_copy(o, c, peer[o]).wait_recv()
        accs = gram(c * span, accs)

    value = dict(zip(pairs, accs))
    for i, k in pairs:
        if i == k:
            dist[i * workers + i] = jnp.zeros((8, LANES), jnp.float32)
        else:
            d = value[i, i] + value[k, k] - 2.0 * value[i, k]
            dist[i * workers + k] = d
            dist[k * workers + i] = d
    lists.wait()
    for i in range(workers):
        s = dist[i * workers + nb_ref[0, i]]
        for j in range(1, nb_ref.shape[0]):
            s = s + dist[i * workers + nb_ref[j, i]]
        part[pl.ds(i, 1), :] = jnp.sum(s, axis=0, keepdims=True)
    column = jnp.sum(part[...], axis=1, keepdims=True)
    line = lax.broadcasted_iota(jnp.int32, (workers, LANES), 0)
    lane = lax.broadcasted_iota(jnp.int32, (workers, LANES), 1)
    mine = plane * workers + me
    score_rows[mine] = jnp.sum(jnp.where(line == lane, column, 0.0), axis=0, keepdims=True)

    def score_copy(o, z):
        return pltpu.make_async_remote_copy(
            src_ref=score_rows.at[mine],
            dst_ref=score_rows.at[mine],
            send_sem=ssend,
            recv_sem=srecv,
            device_id={"worker": peer[o], "mp": (plane + z) % planes},
            device_id_type=MESH,
        )

    def all_scores():
        others = score_rows.at[pl.ds(0, workers * planes - 1)]
        return pltpu.make_async_remote_copy(
            src_ref=others,
            dst_ref=others,
            send_sem=ssend,
            recv_sem=srecv,
            device_id={"worker": peer[1], "mp": plane},
            device_id_type=MESH,
        )

    for o in order:
        for z in range(planes):
            if o or z:
                score_copy(o, z).start()

    if split:
        for ox in rest_order:
            rest_copy(ox, ox - 1).start()
        for ox in rest_order:
            relay_copy(ox).wait_recv()
            add_to_rest(flip(chip, 3 - ox, chips), pl.ds((ox - 1) * half, half), relay[ox - 1])
            rest_copy(3 - ox, ox - 1).start()
    else:
        for ox in rest_order:
            for n in range(2):
                rest_copy(ox, n).start()

    for n in range(2):
        for ox in rest_order:
            rest_copy(ox, n).wait_recv()

    for c in range(CHUNKS):
        at = pl.ds(c * span, span)
        low = rest_in[chip, at, :].astype(jnp.float32)
        for ox in rest_order:
            low = low + rest_recv[ox, at, :].astype(jnp.float32)
        out_ref[at, :] = recv[win_ref[0], at, :].astype(jnp.float32) + low

    all_scores().wait_recv()
    total = jnp.sum(score_rows[...], axis=0) / jnp.float32(total_entries)
    scores_ref[...] = total[:, :workers]

    all_scores().wait_send()
    for ox in range(chips):
        swap(ox).wait_send()
    if split:
        relay_copy(1).wait_send()
        relay_copy(2).wait_send()
    for o in order[:-1]:
        for c in range(CHUNKS):
            gram_copy(o, c, me).wait_send()
    for ox in rest_order:
        for n in range(2):
            rest_copy(ox, n).wait_send()


def emit(scores_ref, block_ref, scores_out, block_out, sems):
    copies = [
        pltpu.make_async_copy(block_ref, block_out, sems.at[0]),
        pltpu.make_async_copy(scores_ref, scores_out, sems.at[1]),
    ]
    for copy in copies:
        copy.start()
    for copy in copies:
        copy.wait()


def solution(mesh):
    workers = mesh.shape["worker"]
    planes = mesh.shape["mp"]
    chips = workers // 2

    def body(gradients, neighbours, winner):
        length = gradients.shape[1]
        rows = length // (LANES * workers)
        entries = neighbours.shape[1] * length * planes
        bf16, f32 = jnp.bfloat16, jnp.float32
        dma = pltpu.SemaphoreType.DMA
        scores, aggregate = pl.pallas_call(
            functools.partial(kernel, workers, planes, entries),
            out_shape=(
                pltpu.VMEM((1, workers), f32),
                pltpu.VMEM((rows, LANES), f32),
            ),
            in_specs=[
                pl.BlockSpec(memory_space=pltpu.HBM),
                pl.BlockSpec(memory_space=pltpu.SMEM),
                pl.BlockSpec(memory_space=pltpu.HBM),
            ],
            out_specs=(
                pl.BlockSpec(memory_space=pltpu.VMEM),
                pl.BlockSpec(memory_space=pltpu.VMEM),
            ),
            scratch_shapes=[
                pltpu.SMEM(neighbours.shape[::-1], jnp.int32),
                pltpu.VMEM((workers, rows, LANES), f32),
                pltpu.VMEM((workers, rows, LANES), bf16),
                pltpu.VMEM((workers, rows, LANES), bf16),
                pltpu.VMEM((2, chips, rows, LANES), bf16),
                pltpu.VMEM((chips, rows, LANES), bf16),
                pltpu.VMEM((chips, rows, LANES), bf16),
                pltpu.VMEM((2, rows // 2, LANES), bf16),
                pltpu.VMEM((workers * workers, 8, LANES), f32),
                pltpu.VMEM((workers, LANES), f32),
                pltpu.VMEM((workers * planes, 1, LANES), f32),
                dma,
                dma((workers, CHUNKS)),
                dma((workers, CHUNKS)),
                dma((workers, CHUNKS)),
                dma((chips,)),
                dma((chips,)),
                dma((2,)),
                dma((2,)),
                dma((chips, 2)),
                dma((chips, 2)),
                dma,
                dma,
            ],
            compiler_params=pltpu.CompilerParams(
                collective_id=0, has_side_effects=True, vmem_limit_bytes=63_500_000
            ),
        )(neighbours.T, winner, gradients.reshape(length // LANES, LANES))
        scores, aggregate = pl.pallas_call(
            emit,
            out_shape=(
                jax.ShapeDtypeStruct(scores.shape, f32),
                jax.ShapeDtypeStruct(aggregate.shape, f32),
            ),
            in_specs=[pl.BlockSpec(memory_space=pltpu.VMEM)] * 2,
            out_specs=(pl.BlockSpec(memory_space=pl.ANY),) * 2,
            scratch_shapes=[dma((2,))],
            compiler_params=pltpu.CompilerParams(vmem_limit_bytes=8 * 1024 * 1024),
        )(scores, aggregate)
        return scores.reshape(workers), aggregate.reshape(rows * LANES)

    in_specs = (P("worker", "mp"), P(), P())
    out_specs = (P(), P(("mp", "worker")))
    return jax.shard_map(body, mesh=mesh, in_specs=in_specs, out_specs=out_specs, check_vma=False)
```

```python
import functools

import jax
import jax.numpy as jnp
from jax import lax
from jax.experimental import pallas as pl
from jax.experimental.pallas import tpu as pltpu
from jax.sharding import PartitionSpec as P

MESH = pl.DeviceIdType.MESH
LANES = 128
CUTS = (0, 2, 4, 6, 8)
PIECES = 2
EARLY = ((), (1, 2), ())


def flip(index, offset, size):
    result, bit = 0, 1
    while bit < size:
        digit = (index // bit) % 2
        if (offset // bit) % 2:
            digit = 1 - digit
        result = result + digit * bit
        bit *= 2
    return result


def kernel(
    workers,
    planes,
    total_entries,
    nb_hbm,
    win_ref,
    g_ref,
    scores_ref,
    out_ref,
    nb_ref,
    stage,
    rounded,
    recv,
    rest,
    rest_in,
    rest_recv,
    relay,
    dist,
    part,
    score_rows,
    small_sem,
    load_sem,
    gsend,
    grecv,
    osend,
    orecv,
    ysend,
    yrecv,
    rsend,
    rrecv,
    ssend,
    srecv,
    hello,
    chip_hello,
    lines,
):
    me = lax.axis_index("worker")
    plane = lax.axis_index("mp")
    core = me % 2
    chip = me // 2
    chips = workers // 2
    rows = stage.shape[1]
    starts = [rows * cut // CUTS[-1] for cut in CUTS]
    chunks = [pl.ds(a, b - a) for a, b in zip(starts, starts[1:])]
    bits = max(chips.bit_length() - 1, 0)

    def far(o):
        return bin(o // 2).count("1")

    order = sorted(range(2, workers), key=lambda o: (far(o), o // 2, o % 2)) + [1, 0]
    near = [o for o in range(1, workers) if far(o) < 2]
    peer = [flip(me, o, workers) for o in range(workers)]

    barrier = pltpu.get_barrier_semaphore()
    for o in near:
        pl.semaphore_signal(barrier, inc=1, device_id={"worker": peer[o]}, device_id_type=MESH)
    below, above = plane > 0, plane < planes - 1
    for there, step in ((below, -1), (above, 1)):

        @pl.when(there)
        def _(step=step):
            pl.semaphore_signal(
                barrier, inc=1, device_id={"mp": plane + step}, device_id_type=MESH
            )

    entered = len(near) + below.astype(jnp.int32) + above.astype(jnp.int32)

    def tell_chips(distance):
        for b in range(bits - distance):
            pl.semaphore_signal(
                chip_hello.at[distance - 1],
                inc=1,
                device_id={"worker": peer[2 << b]},
                device_id_type=MESH,
            )

    def hear_chips(distance):
        if bits > distance:
            pl.semaphore_wait(chip_hello.at[distance - 1], bits - distance)

    def tell(distance):
        if distance > planes - 2:
            return
        for n, step in ((0, -1), (1, 1)):
            to, seen = plane + step, plane - step * distance

            @pl.when((0 <= to) & (to < planes) & (0 <= seen) & (seen < planes))
            def _(n=n, to=to):
                pl.semaphore_signal(
                    hello.at[n, distance - 1], inc=1, device_id={"mp": to}, device_id_type=MESH
                )

    def hear(distance):
        for n, step in ((0, 1), (1, -1)):
            seen = plane + step * (distance + 1)

            @pl.when((0 <= seen) & (seen < planes))
            def _(n=n):
                pl.semaphore_wait(hello.at[n, distance - 1], 1)

    for c, at in enumerate(chunks):
        for o in order:
            first = pl.multiple_of(peer[o] * rows, rows) + at.start
            pltpu.make_async_copy(
                g_ref.at[pl.ds(first, at.size), :], stage.at[o, at, :], load_sem.at[c]
            ).start()
    lists = pltpu.make_async_copy(nb_hbm, nb_ref, small_sem)
    lists.start()

    def to_peer(o, src, dst, send_sem, recv_sem):
        return pltpu.make_async_remote_copy(
            src_ref=src,
            dst_ref=dst,
            send_sem=send_sem,
            recv_sem=recv_sem,
            device_id={"worker": peer[o]},
            device_id_type=MESH,
        )

    def gram_copy(o, c):
        at = chunks[c]
        return to_peer(o, rounded.at[o, at, :], recv.at[me, at, :], gsend, grecv.at[c])

    def gram_chunk(c):
        whole = recv.at[pl.ds(0, workers - 1), chunks[c], :]
        return to_peer(1, whole, whole, gsend, grecv.at[c])

    keep = jnp.where(win_ref[0] == me, 1.0, 0.0).astype(jnp.float32)

    def convert(o, at):
        x = stage[o, at, :]
        hi = x.astype(jnp.bfloat16)
        if o == 0:
            recv[me, at, :] = hi
        else:
            rounded[o, at, :] = hi
        low = ((x - hi.astype(jnp.float32)) * keep).astype(jnp.bfloat16)
        rest[peer[o] % 2, peer[o] // 2, at, :] = low

    def swap(ox):
        there = flip(chip, ox, chips)
        return to_peer(1, rest.at[1 - core, there], rest_in.at[there], osend, orecv)

    def add_to_rest(there, at, other):
        rest_in[there, at, :] = rest_in[there, at, :] + other

    def combine(ox):
        there = flip(chip, ox, chips)
        for at in chunks:
            add_to_rest(there, at, rest[core, there, at, :])

    split = chips == 4
    half = rows // 2
    piece = half // PIECES

    def relay_copy(ox, p):
        at = pl.ds(p * piece, piece)
        return to_peer(
            2 * ox,
            rest_in.at[flip(chip, 3, chips), pl.ds((ox - 1) * half + p * piece, piece), :],
            relay.at[ox - 1, at, :],
            ysend,
            yrecv.at[ox - 1, p],
        )

    def rest_copy(ox, n, p):
        at = pl.ds(n * half + p * piece, piece)
        return to_peer(
            2 * ox,
            rest_in.at[flip(chip, ox, chips), at, :],
            rest_recv.at[ox, at, :],
            rsend,
            rrecv,
        )

    rest_order = sorted(range(1, chips), key=lambda ox: bin(ox).count("1"))
    if split:
        rest_order = [1, 2]

    first, reach = True, 1
    for c, at in enumerate(chunks):
        pltpu.make_async_copy(stage.at[:, at, :], stage.at[:, at, :], load_sem.at[c]).wait()
        for o in order:
            convert(o, at)
            if first:
              pl.semaphore_wait(barrier, entered)
              tell_chips(1)
              tell(1)
              first = False
            if c == 0 and far(o) > reach:
                for distance in range(reach, far(o)):
                  hear_chips(distance)
                  tell_chips(distance + 1)
                reach = far(o)
            if o:
                gram_copy(o, c).start()
    for ox in range(chips):
        swap(ox).start()

    to_peer(1, rest_in, rest_in, osend, orecv).wait_recv()
    for ox in reversed(range(chips)):
        combine(ox)

    def early(ox):
        for p in range(PIECES):
            relay_copy(ox, p).start()
        for p in range(PIECES):
            rest_copy(ox, ox - 1, p).start()

    if split:
        for n in EARLY[0]:
            early(n)

    pairs = [(i, k) for i in range(workers) for k in range(i, workers)]

    def gram(rows_at, accs):
        def one(step, accs):
            at = pl.ds(pl.multiple_of(rows_at.start + step * 16, 16), 16)
            xs = [recv[i, at, :].astype(jnp.float32) for i in range(workers)]
            lo = [x[:8] for x in xs]
            hi = [x[8:] for x in xs]
            return tuple(
                a + (lo[i] * lo[k] + hi[i] * hi[k]) for a, (i, k) in zip(accs, pairs)
            )

        return lax.fori_loop(0, rows_at.size // 16, one, accs)

    accs = tuple(jnp.zeros((8, LANES), jnp.float32) for _ in pairs)
    for c, at in enumerate(chunks):
        if split and c == len(chunks) - 1:
            for n in EARLY[1]:
                early(n)
        gram_chunk(c).wait_recv()
        accs = gram(at, accs)
        if c == 0:
            for distance in range(1, planes - 1):
                hear(distance)
                tell(distance + 1)
            for o in range(1, workers):
                pl.semaphore_signal(
                    lines, inc=1, device_id={"worker": peer[o]}, device_id_type=MESH
                )

    value = dict(zip(pairs, accs))
    for i, k in pairs:
        if i == k:
            dist[i * workers + i] = jnp.zeros((8, LANES), jnp.float32)
        else:
            d = value[i, i] + value[k, k] - 2.0 * value[i, k]
            dist[i * workers + k] = d
            dist[k * workers + i] = d
    lists.wait()
    for i in range(workers):
        s = dist[i * workers + nb_ref[0, i]]
        for j in range(1, nb_ref.shape[0]):
            s = s + dist[i * workers + nb_ref[j, i]]
        part[pl.ds(i, 1), :] = jnp.sum(s, axis=0, keepdims=True)
    column = jnp.sum(part[...], axis=1, keepdims=True)
    line = lax.broadcasted_iota(jnp.int32, (workers, LANES), 0)
    lane = lax.broadcasted_iota(jnp.int32, (workers, LANES), 1)
    mine = plane * workers + me
    score_rows[mine] = jnp.sum(jnp.where(line == lane, column, 0.0), axis=0, keepdims=True)

    def score_copy(o, z):
        return pltpu.make_async_remote_copy(
            src_ref=score_rows.at[mine],
            dst_ref=score_rows.at[mine],
            send_sem=ssend,
            recv_sem=srecv,
            device_id={"worker": peer[o], "mp": (plane + z) % planes},
            device_id_type=MESH,
        )

    def all_scores():
        others = score_rows.at[pl.ds(0, workers * planes - 1)]
        return pltpu.make_async_remote_copy(
            src_ref=others,
            dst_ref=others,
            send_sem=ssend,
            recv_sem=srecv,
            device_id={"worker": peer[1], "mp": plane},
            device_id_type=MESH,
        )

    pl.semaphore_wait(lines, workers - 1)
    for o in order:
        for z in range(planes):
            if o or z:
                score_copy(o, z).start()

    if split:
        for n in EARLY[2]:
            early(n)
    if split:
        for p in range(PIECES):
            for ox in rest_order:
                relay_copy(ox, p).wait_recv()
                at = pl.ds((ox - 1) * half + p * piece, piece)
                add_to_rest(flip(chip, 3 - ox, chips), at, relay[ox - 1, pl.ds(p * piece, piece), :])
                rest_copy(3 - ox, ox - 1, p).start()
    else:
        for ox in rest_order:
            for n in range(2):
                for p in range(PIECES):
                    rest_copy(ox, n, p).start()

    arrived = rest_recv.at[pl.ds(0, len(rest_order))]
    to_peer(1, arrived, arrived, rsend, rrecv).wait_recv()

    for at in chunks:
        low = rest_in[chip, at, :].astype(jnp.float32)
        for ox in rest_order:
            low = low + rest_recv[ox, at, :].astype(jnp.float32)
        out_ref[at, :] = recv[win_ref[0], at, :].astype(jnp.float32) + low

    all_scores().wait_recv()
    total = jnp.sum(score_rows[...], axis=0) / jnp.float32(total_entries)
    scores_ref[...] = total[:, :workers]

    all_scores().wait_send()
    to_peer(1, rest_in, rest_in, osend, orecv).wait_send()
    if split:
        to_peer(1, relay, relay, ysend, yrecv.at[0, 0]).wait_send()
    sent = rounded.at[pl.ds(0, workers - 1)]
    to_peer(1, sent, sent, gsend, grecv.at[0]).wait_send()
    to_peer(1, arrived, arrived, rsend, rrecv).wait_send()


def emit(scores_ref, block_ref, scores_out, block_out, sems):
    copies = [
        pltpu.make_async_copy(block_ref, block_out, sems.at[0]),
        pltpu.make_async_copy(scores_ref, scores_out, sems.at[1]),
    ]
    for copy in copies:
        copy.start()
    for copy in copies:
        copy.wait()


def solution(mesh):
    workers = mesh.shape["worker"]
    planes = mesh.shape["mp"]
    chips = workers // 2

    def body(gradients, neighbours, winner):
        length = gradients.shape[1]
        rows = length // (LANES * workers)
        entries = neighbours.shape[1] * length * planes
        bf16, f32 = jnp.bfloat16, jnp.float32
        dma = pltpu.SemaphoreType.DMA
        scores, aggregate = pl.pallas_call(
            functools.partial(kernel, workers, planes, entries),
            out_shape=(
                pltpu.VMEM((1, workers), f32),
                pltpu.VMEM((rows, LANES), f32),
            ),
            in_specs=[
                pl.BlockSpec(memory_space=pltpu.HBM),
                pl.BlockSpec(memory_space=pltpu.SMEM),
                pl.BlockSpec(memory_space=pltpu.HBM),
            ],
            out_specs=(
                pl.BlockSpec(memory_space=pltpu.VMEM),
                pl.BlockSpec(memory_space=pltpu.VMEM),
            ),
            scratch_shapes=[
                pltpu.SMEM(neighbours.shape[::-1], jnp.int32),
                pltpu.VMEM((workers, rows, LANES), f32),
                pltpu.VMEM((workers, rows, LANES), bf16),
                pltpu.VMEM((workers, rows, LANES), bf16),
                pltpu.VMEM((2, chips, rows, LANES), bf16),
                pltpu.VMEM((chips, rows, LANES), bf16),
                pltpu.VMEM((chips, rows, LANES), bf16),
                pltpu.VMEM((2, rows // 2, LANES), bf16),
                pltpu.VMEM((workers * workers, 8, LANES), f32),
                pltpu.VMEM((workers, LANES), f32),
                pltpu.VMEM((workers * planes, 1, LANES), f32),
                dma,
                dma((len(CUTS) - 1,)),
                dma,
                dma((len(CUTS) - 1,)),
                dma,
                dma,
                dma,
                dma((2, PIECES)),
                dma,
                dma,
                dma,
                dma,
                pltpu.SemaphoreType.REGULAR((2, max(planes - 2, 1))),
                pltpu.SemaphoreType.REGULAR((max(chips.bit_length() - 2, 1),)),
                pltpu.SemaphoreType.REGULAR,
            ],
            compiler_params=pltpu.CompilerParams(
                collective_id=0, has_side_effects=True, vmem_limit_bytes=63_500_000
            ),
        )(neighbours.T, winner, gradients.reshape(length // LANES, LANES))
        scores, aggregate = pl.pallas_call(
            emit,
            out_shape=(
                jax.ShapeDtypeStruct(scores.shape, f32),
                jax.ShapeDtypeStruct(aggregate.shape, f32),
            ),
            in_specs=[pl.BlockSpec(memory_space=pltpu.VMEM)] * 2,
            out_specs=(pl.BlockSpec(memory_space=pl.ANY),) * 2,
            scratch_shapes=[dma((2,))],
            compiler_params=pltpu.CompilerParams(vmem_limit_bytes=8 * 1024 * 1024),
        )(scores, aggregate)
        return scores.reshape(workers), aggregate.reshape(rows * LANES)

    in_specs = (P("worker", "mp"), P(), P())
    out_specs = (P(), P(("mp", "worker")))
    return jax.shard_map(body, mesh=mesh, in_specs=in_specs, out_specs=out_specs, check_vma=False)
```

```python
import functools

import jax
import jax.numpy as jnp
from jax import lax
from jax.experimental import pallas as pl
from jax.experimental.pallas import tpu as pltpu
from jax.sharding import PartitionSpec as P

MESH = pl.DeviceIdType.MESH
LANES = 128
CHUNKS = 4
SHIFT = 3 / 32
TILE = 16
PIECES = 2


def flip(index, offset, size):
    result, bit = 0, 1
    while bit < size:
        digit = (index // bit) % 2
        if (offset // bit) % 2:
            digit = 1 - digit
        result = result + digit * bit
        bit *= 2
    return result


def cuts(rows, shift):
    first = int(rows * SHIFT) // TILE * TILE if shift else 0
    ends = [first + (rows - first) * n // CHUNKS // TILE * TILE for n in range(1, CHUNKS + 1)]
    return ([0, first] if shift else [0]) + ends


def kernel(
    workers,
    planes,
    total_entries,
    nb_hbm,
    win_ref,
    g_ref,
    scores_ref,
    out_ref,
    nb_ref,
    stage,
    rounded,
    recv,
    rest,
    rest_in,
    rest_recv,
    relay,
    dist,
    part,
    score_rows,
    moved_in,
    extra,
    small_sem,
    load_sem,
    gsend,
    grecv,
    osend,
    orecv,
    ysend,
    yrecv,
    rsend,
    rrecv,
    ssend,
    srecv,
    zsend,
    zrecv,
    fsend,
    frecv,
    risen,
    chip_hello,
    lines,
):
    me = lax.axis_index("worker")
    plane = lax.axis_index("mp")
    core = me % 2
    chip = me // 2
    chips = workers // 2
    rows = stage.shape[1]
    split = chips == 4
    shift = split and planes == 4
    donor, helper, eager = planes - 1, planes - 3, 0
    starts = cuts(rows, shift)
    chunks = [pl.ds(a, b - a) for a, b in zip(starts, starts[1:])]
    moved = chunks[0]
    bits = max(chips.bit_length() - 1, 0)

    def far(o):
        return bin(o // 2).count("1")

    order = sorted(range(2, workers), key=lambda o: (far(o), o // 2, o % 2)) + [1, 0]
    near = [o for o in range(1, workers) if far(o) < 2]
    peer = [flip(me, o, workers) for o in range(workers)]

    barrier = pltpu.get_barrier_semaphore()
    for o in near:
        pl.semaphore_signal(barrier, inc=1, device_id={"worker": peer[o]}, device_id_type=MESH)
    for p in range(1, planes):

        @pl.when(plane < p)
        def _(p=p):
            pl.semaphore_signal(barrier, inc=1, device_id={"mp": p}, device_id_type=MESH)

    entered = len(near) + plane

    def tell_chips(distance):
        for b in range(bits - distance):
            pl.semaphore_signal(
                chip_hello.at[distance - 1],
                inc=1,
                device_id={"worker": peer[2 << b]},
                device_id_type=MESH,
            )

    def hear_chips(distance):
        if bits > distance:
            pl.semaphore_wait(chip_hello.at[distance - 1], bits - distance)

    def tell_below():
        for p in range(planes - 1):

            @pl.when(p < plane)
            def _(p=p):
                pl.semaphore_signal(risen, inc=1, device_id={"mp": p}, device_id_type=MESH)

    for c, at in enumerate(chunks):
        for o in order:
            first = pl.multiple_of(peer[o] * rows, rows) + at.start
            pltpu.make_async_copy(
                g_ref.at[pl.ds(first, at.size), :], stage.at[o, at, :], load_sem.at[c]
            ).start()
    lists = pltpu.make_async_copy(nb_hbm, nb_ref, small_sem)
    lists.start()

    def to_peer(o, src, dst, send_sem, recv_sem):
        return pltpu.make_async_remote_copy(
            src_ref=src,
            dst_ref=dst,
            send_sem=send_sem,
            recv_sem=recv_sem,
            device_id={"worker": peer[o]},
            device_id_type=MESH,
        )

    def gram_copy(o, c):
        at = chunks[c]
        return to_peer(o, rounded.at[o, at, :], recv.at[me, at, :], gsend, grecv.at[c])

    def gram_chunk(c):
        whole = recv.at[pl.ds(0, workers - 1), chunks[c], :]
        return to_peer(1, whole, whole, gsend, grecv.at[c])

    keep = jnp.where(win_ref[0] == me, 1.0, 0.0).astype(jnp.float32)

    def convert(o, at):
        x = stage[o, at, :]
        hi = x.astype(jnp.bfloat16)
        if o == 0:
            recv[me, at, :] = hi
        if o or (shift and at is moved):
            rounded[o, at, :] = hi
        low = ((x - hi.astype(jnp.float32)) * keep).astype(jnp.bfloat16)
        rest[peer[o] % 2, peer[o] // 2, at, :] = low

    def swap(ox):
        there = flip(chip, ox, chips)
        return to_peer(1, rest.at[1 - core, there], rest_in.at[there], osend, orecv)

    def add_to_rest(there, at, other):
        rest_in[there, at, :] = rest_in[there, at, :] + other

    def combine(ox):
        there = flip(chip, ox, chips)
        for at in chunks:
            add_to_rest(there, at, rest[core, there, at, :])

    half = rows // 2
    piece = half // PIECES

    def relay_copy(ox, p):
        at = pl.ds(p * piece, piece)
        return to_peer(
            2 * ox,
            rest_in.at[flip(chip, 3, chips), pl.ds((ox - 1) * half + p * piece, piece), :],
            relay.at[ox - 1, at, :],
            ysend,
            yrecv.at[ox - 1, p],
        )

    def rest_copy(ox, n, p):
        at = pl.ds(n * half + p * piece, piece)
        return to_peer(
            2 * ox,
            rest_in.at[flip(chip, ox, chips), at, :],
            rest_recv.at[ox, at, :],
            rsend,
            rrecv,
        )

    rest_order = sorted(range(1, chips), key=lambda ox: bin(ox).count("1"))
    if split:
        rest_order = [1, 2]

    def send(c, peers):
        def start():
            for o in peers:
                gram_copy(o, c).start()

        if shift and c == 0:
            pl.when(plane != donor)(start)
        elif shift and c == len(chunks) - 1:
            pl.when(plane != eager)(start)
        else:
            start()

    def to_helper():
        return pltpu.make_async_remote_copy(
            src_ref=rounded.at[:, moved, :],
            dst_ref=moved_in,
            send_sem=zsend,
            recv_sem=zrecv,
            device_id={"mp": helper},
            device_id_type=MESH,
        )

    close = [o for o in order if o and far(o) < 2]
    distant = [o for o in order if far(o) >= 2]
    lead = 2 if shift else 1
    for c, at in enumerate(chunks):
        pltpu.make_async_copy(stage.at[:, at, :], stage.at[:, at, :], load_sem.at[c]).wait()
        for o in order:
            convert(o, at)
        if c == 0:
          pl.semaphore_wait(barrier, entered)
          tell_chips(1)
          tell_below()
        send(c, close)
        if c == lead - 1:
          for distance in range(1, bits):
              hear_chips(distance)
              tell_chips(distance + 1)
          for late in range(lead):
              send(late, distant)
        elif c >= lead:
            send(c, distant)
        if shift and c == 0:

            @pl.when(plane == donor)
            def _():
                to_helper().start()
    if shift:

        @pl.when(plane == donor)
        def _():
            for o in close + distant:
                gram_copy(o, 0).start()

    for ox in range(chips):
        swap(ox).start()

    to_peer(1, rest_in, rest_in, osend, orecv).wait_recv()
    for ox in reversed(range(chips)):
        combine(ox)

    def relay_piece(p):
        for ox in rest_order:
            relay_copy(ox, p).start()

    def own_halves():
        for p in range(PIECES):
            for ox in rest_order:
                rest_copy(ox, ox - 1, p).start()

    def pass_on(p):
        for ox in rest_order:
            relay_copy(ox, p).wait_recv()
            at = pl.ds(p * piece, piece)
            there = flip(chip, 3 - ox, chips)
            add_to_rest(there, pl.ds((ox - 1) * half + p * piece, piece), relay[ox - 1, at, :])
            rest_copy(3 - ox, ox - 1, p).start()

    if shift:

        @pl.when(plane == eager)
        def _():
            relay_piece(0)
            for o in close + distant:
                gram_copy(o, len(chunks) - 1).start()

    pairs = [(i, k) for i in range(workers) for k in range(i, workers)]

    def gram(ref, at, accs, active=None):
        def one(step, accs):
            part_at = pl.ds(pl.multiple_of(at.start + step * TILE, TILE), TILE)
            xs = [ref[i, part_at, :].astype(jnp.float32) for i in range(workers)]
            lo = [x[:8] for x in xs]
            hi = [x[8:] for x in xs]
            return tuple(
                a + (lo[i] * lo[k] + hi[i] * hi[k]) for a, (i, k) in zip(accs, pairs)
            )

        steps = at.size // TILE
        if active is not None:
            steps = steps * active.astype(jnp.int32)
        return lax.fori_loop(0, steps, one, accs)

    def forward(o):
        return to_peer(o, moved_in.at[o], extra.at[me], fsend, frecv)

    def forwarded():
        whole = extra.at[pl.ds(0, workers - 1)]
        return to_peer(1, whole, whole, fsend, frecv)

    accs = tuple(jnp.zeros((8, LANES), jnp.float32) for _ in pairs)
    for c, at in enumerate(chunks):
        if shift and c == len(chunks) - 2:

            @pl.when(plane == helper)
            def _():
              to_helper().wait_recv()
              for o in close + distant:
                  forward(o).start()
              extra[me] = moved_in[0]

        if split and c == len(chunks) - 1:
            if shift:
                pl.when(plane != eager)(lambda: relay_piece(0))
            else:
                relay_piece(0)
            for p in range(1, PIECES):
                relay_piece(p)
            own_halves()
            if shift:
                pl.when(plane == eager)(lambda: pass_on(0))
        if shift and c == 0:
          pl.when(plane != donor)(gram_chunk(c).wait_recv)
          accs = gram(recv, at, accs, plane != donor)
        else:
          gram_chunk(c).wait_recv()
          accs = gram(recv, at, accs)
        if c == 0:

            @pl.when(plane < planes - 1)
            def _():
                pl.semaphore_wait(risen, planes - 1 - plane)

            for o in range(1, workers):
                pl.semaphore_signal(
                    lines, inc=1, device_id={"worker": peer[o]}, device_id_type=MESH
                )
    if shift:
      pl.when(plane == helper)(forwarded().wait_recv)
      accs = gram(extra, pl.ds(0, moved.size), accs, plane == helper)

    value = dict(zip(pairs, accs))
    for i, k in pairs:
        if i == k:
            dist[i * workers + i] = jnp.zeros((8, LANES), jnp.float32)
        else:
            d = value[i, i] + value[k, k] - 2.0 * value[i, k]
            dist[i * workers + k] = d
            dist[k * workers + i] = d
    lists.wait()
    for i in range(workers):
        s = dist[i * workers + nb_ref[0, i]]
        for j in range(1, nb_ref.shape[0]):
            s = s + dist[i * workers + nb_ref[j, i]]
        part[pl.ds(i, 1), :] = jnp.sum(s, axis=0, keepdims=True)
    column = jnp.sum(part[...], axis=1, keepdims=True)
    line = lax.broadcasted_iota(jnp.int32, (workers, LANES), 0)
    lane = lax.broadcasted_iota(jnp.int32, (workers, LANES), 1)
    mine = plane * workers + me
    score_rows[mine] = jnp.sum(jnp.where(line == lane, column, 0.0), axis=0, keepdims=True)

    def score_copy(o, to):
        return pltpu.make_async_remote_copy(
            src_ref=score_rows.at[mine],
            dst_ref=score_rows.at[mine],
            send_sem=ssend,
            recv_sem=srecv,
            device_id={"worker": peer[o], "mp": to},
            device_id_type=MESH,
        )

    def all_scores():
        others = score_rows.at[pl.ds(0, workers * planes - 1)]
        return pltpu.make_async_remote_copy(
            src_ref=others,
            dst_ref=others,
            send_sem=ssend,
            recv_sem=srecv,
            device_id={"worker": peer[1], "mp": plane},
            device_id_type=MESH,
        )

    pl.semaphore_wait(lines, workers - 1)
    for to in range(planes):
        for o in order[:-1]:
            score_copy(o, to).start()

        @pl.when(plane != to)
        def _(to=to):
            score_copy(0, to).start()

    if split:
        if shift:
            pl.when(plane != eager)(lambda: pass_on(0))
        else:
            pass_on(0)
        for p in range(1, PIECES):
            pass_on(p)
    else:
        for ox in rest_order:
            for n in range(2):
                for p in range(PIECES):
                    rest_copy(ox, n, p).start()

    arrived = rest_recv.at[pl.ds(0, len(rest_order))]
    to_peer(1, arrived, arrived, rsend, rrecv).wait_recv()

    if shift:
        pl.when(plane == donor)(gram_chunk(0).wait_recv)
    for at in chunks:
        low = rest_in[chip, at, :].astype(jnp.float32)
        for ox in rest_order:
            low = low + rest_recv[ox, at, :].astype(jnp.float32)
        out_ref[at, :] = recv[win_ref[0], at, :].astype(jnp.float32) + low

    all_scores().wait_recv()
    total = jnp.sum(score_rows[...], axis=0) / jnp.float32(total_entries)
    scores_ref[...] = total[:, :workers]

    all_scores().wait_send()
    to_peer(1, rest_in, rest_in, osend, orecv).wait_send()
    if split:
        to_peer(1, relay, relay, ysend, yrecv.at[0, 0]).wait_send()
    sent = rounded.at[pl.ds(0, workers - 1)]
    to_peer(1, sent, sent, gsend, grecv.at[0]).wait_send()
    if shift:
        pl.when(plane == donor)(to_helper().wait_send)
        pl.when(plane == helper)(forwarded().wait_send)
    to_peer(1, arrived, arrived, rsend, rrecv).wait_send()


def emit(scores_ref, block_ref, scores_out, block_out, sems):
    copies = [
        pltpu.make_async_copy(block_ref, block_out, sems.at[0]),
        pltpu.make_async_copy(scores_ref, scores_out, sems.at[1]),
    ]
    for copy in copies:
        copy.start()
    for copy in copies:
        copy.wait()


def solution(mesh):
    workers = mesh.shape["worker"]
    planes = mesh.shape["mp"]
    chips = workers // 2

    def body(gradients, neighbours, winner):
        length = gradients.shape[1]
        rows = length // (LANES * workers)
        starts = cuts(rows, chips == 4 and planes == 4)
        entries = neighbours.shape[1] * length * planes
        bf16, f32 = jnp.bfloat16, jnp.float32
        dma = pltpu.SemaphoreType.DMA
        scores, aggregate = pl.pallas_call(
            functools.partial(kernel, workers, planes, entries),
            out_shape=(
                pltpu.VMEM((1, workers), f32),
                pltpu.VMEM((rows, LANES), f32),
            ),
            in_specs=[
                pl.BlockSpec(memory_space=pltpu.HBM),
                pl.BlockSpec(memory_space=pltpu.SMEM),
                pl.BlockSpec(memory_space=pltpu.HBM),
            ],
            out_specs=(
                pl.BlockSpec(memory_space=pltpu.VMEM),
                pl.BlockSpec(memory_space=pltpu.VMEM),
            ),
            scratch_shapes=[
                pltpu.SMEM(neighbours.shape[::-1], jnp.int32),
                pltpu.VMEM((workers, rows, LANES), f32),
                pltpu.VMEM((workers, rows, LANES), bf16),
                pltpu.VMEM((workers, rows, LANES), bf16),
                pltpu.VMEM((2, chips, rows, LANES), bf16),
                pltpu.VMEM((chips, rows, LANES), bf16),
                pltpu.VMEM((chips, rows, LANES), bf16),
                pltpu.VMEM((2, rows // 2, LANES), bf16),
                pltpu.VMEM((workers * workers, 8, LANES), f32),
                pltpu.VMEM((workers, LANES), f32),
                pltpu.VMEM((workers * planes, 1, LANES), f32),
                pltpu.VMEM((workers, starts[1], LANES), bf16),
                pltpu.VMEM((workers, starts[1], LANES), bf16),
                dma,
                dma((len(starts) - 1,)),
                dma,
                dma((len(starts) - 1,)),
                dma,
                dma,
                dma,
                dma((2, PIECES)),
                dma,
                dma,
                dma,
                dma,
                dma,
                dma,
                dma,
                dma,
                pltpu.SemaphoreType.REGULAR,
                pltpu.SemaphoreType.REGULAR((max(chips.bit_length() - 2, 1),)),
                pltpu.SemaphoreType.REGULAR,
            ],
            compiler_params=pltpu.CompilerParams(
                collective_id=0, has_side_effects=True, vmem_limit_bytes=63_500_000
            ),
        )(neighbours.T, winner, gradients.reshape(length // LANES, LANES))
        scores, aggregate = pl.pallas_call(
            emit,
            out_shape=(
                jax.ShapeDtypeStruct(scores.shape, f32),
                jax.ShapeDtypeStruct(aggregate.shape, f32),
            ),
            in_specs=[pl.BlockSpec(memory_space=pltpu.VMEM)] * 2,
            out_specs=(pl.BlockSpec(memory_space=pl.ANY),) * 2,
            scratch_shapes=[dma((2,))],
            compiler_params=pltpu.CompilerParams(vmem_limit_bytes=8 * 1024 * 1024),
        )(scores, aggregate)
        return scores.reshape(workers), aggregate.reshape(rows * LANES)

    in_specs = (P("worker", "mp"), P(), P())
    out_specs = (P(), P(("mp", "worker")))
    return jax.shard_map(body, mesh=mesh, in_specs=in_specs, out_specs=out_specs, check_vma=False)
```

```python
import functools

import jax
import jax.numpy as jnp
from jax import lax
from jax.experimental import pallas as pl
from jax.experimental.pallas import tpu as pltpu
from jax.sharding import PartitionSpec as P

MESH = pl.DeviceIdType.MESH
LANES = 128
CHUNKS = 4
SHARES = (1, 2)
PARTS = 32
TILE = 16
PIECES = 2


def flip(index, offset, size):
    result, bit = 0, 1
    while bit < size:
        digit = (index // bit) % 2
        if (offset // bit) % 2:
            digit = 1 - digit
        result = result + digit * bit
        bit *= 2
    return result


def shares(rows, chips, planes):
    unit = rows // PARTS // TILE * TILE
    return [unit * n for n in SHARES] if chips == planes == 4 and unit else []


def cuts(rows, given):
    first = sum(given)
    ends = [first + (rows - first) * n // CHUNKS // TILE * TILE for n in range(1, CHUNKS + 1)]
    return ([0, first] if first else [0]) + ends


def kernel(
    workers,
    planes,
    total_entries,
    nb_hbm,
    win_ref,
    g_ref,
    scores_ref,
    out_ref,
    nb_ref,
    stage,
    rounded,
    recv,
    rest,
    rest_in,
    rest_recv,
    relay,
    dist,
    part,
    score_rows,
    moved_in,
    extra,
    small_sem,
    load_sem,
    gsend,
    grecv,
    osend,
    orecv,
    ysend,
    yrecv,
    rsend,
    rrecv,
    ssend,
    srecv,
    zsend,
    zrecv,
    fsend,
    frecv,
    risen,
    chip_hello,
    lines,
):
    me = lax.axis_index("worker")
    plane = lax.axis_index("mp")
    core = me % 2
    chip = me // 2
    chips = workers // 2
    rows = stage.shape[1]
    split = chips == 4
    given = shares(rows, chips, planes)
    shift = bool(given)
    donor, eager = planes - 1, 0
    starts = cuts(rows, given)
    chunks = [pl.ds(a, b - a) for a, b in zip(starts, starts[1:])]
    moved = chunks[0]
    bits = max(chips.bit_length() - 1, 0)

    def far(o):
        return bin(o // 2).count("1")

    order = sorted(range(2, workers), key=lambda o: (far(o), o // 2, o % 2)) + [1, 0]
    near = [o for o in range(1, workers) if far(o) < 2]
    peer = [flip(me, o, workers) for o in range(workers)]

    barrier = pltpu.get_barrier_semaphore()
    for o in near:
        pl.semaphore_signal(barrier, inc=1, device_id={"worker": peer[o]}, device_id_type=MESH)
    for p in range(1, planes):

        @pl.when(plane < p)
        def _(p=p):
            pl.semaphore_signal(barrier, inc=1, device_id={"mp": p}, device_id_type=MESH)

    entered = len(near) + plane

    def tell_chips(distance):
        for b in range(bits - distance):
            pl.semaphore_signal(
                chip_hello.at[distance - 1],
                inc=1,
                device_id={"worker": peer[2 << b]},
                device_id_type=MESH,
            )

    def hear_chips(distance):
        if bits > distance:
            pl.semaphore_wait(chip_hello.at[distance - 1], bits - distance)

    def tell_below():
        for p in range(planes - 1):

            @pl.when(p < plane)
            def _(p=p):
                pl.semaphore_signal(risen, inc=1, device_id={"mp": p}, device_id_type=MESH)

    turns = [1, 0] + list(range(2, len(chunks))) if shift else list(range(len(chunks)))
    for c in turns:
        at = chunks[c]
        for o in order:
            first = pl.multiple_of(peer[o] * rows, rows) + at.start
            pltpu.make_async_copy(
                g_ref.at[pl.ds(first, at.size), :], stage.at[o, at, :], load_sem.at[c]
            ).start()
    lists = pltpu.make_async_copy(nb_hbm, nb_ref, small_sem)
    lists.start()

    def to_peer(o, src, dst, send_sem, recv_sem):
        return pltpu.make_async_remote_copy(
            src_ref=src,
            dst_ref=dst,
            send_sem=send_sem,
            recv_sem=recv_sem,
            device_id={"worker": peer[o]},
            device_id_type=MESH,
        )

    def gram_copy(o, c):
        at = chunks[c]
        return to_peer(o, rounded.at[o, at, :], recv.at[me, at, :], gsend, grecv.at[c])

    def gram_chunk(c):
        whole = recv.at[pl.ds(0, workers - 1), chunks[c], :]
        return to_peer(1, whole, whole, gsend, grecv.at[c])

    keep = jnp.where(win_ref[0] == me, 1.0, 0.0).astype(jnp.float32)

    def convert(o, at):
        x = stage[o, at, :]
        hi = x.astype(jnp.bfloat16)
        if o == 0:
            recv[me, at, :] = hi
        if o or (shift and at is moved):
            rounded[o, at, :] = hi
        low = ((x - hi.astype(jnp.float32)) * keep).astype(jnp.bfloat16)
        rest[peer[o] % 2, peer[o] // 2, at, :] = low

    def swap(ox):
        there = flip(chip, ox, chips)
        return to_peer(1, rest.at[1 - core, there], rest_in.at[there], osend, orecv)

    def add_to_rest(there, at, other):
        rest_in[there, at, :] = rest_in[there, at, :] + other

    def combine(ox):
        there = flip(chip, ox, chips)
        for at in chunks:
            add_to_rest(there, at, rest[core, there, at, :])

    half = rows // 2
    piece = half // PIECES

    def relay_copy(ox, p):
        at = pl.ds(p * piece, piece)
        return to_peer(
            2 * ox,
            rest_in.at[flip(chip, 3, chips), pl.ds((ox - 1) * half + p * piece, piece), :],
            relay.at[ox - 1, at, :],
            ysend,
            yrecv.at[ox - 1, p],
        )

    def rest_copy(ox, n, p):
        at = pl.ds(n * half + p * piece, piece)
        return to_peer(
            2 * ox,
            rest_in.at[flip(chip, ox, chips), at, :],
            rest_recv.at[ox, at, :],
            rsend,
            rrecv,
        )

    rest_order = sorted(range(1, chips), key=lambda ox: bin(ox).count("1"))
    if split:
        rest_order = [1, 2]

    def send(c, peers):
        def start():
            for o in peers:
                gram_copy(o, c).start()

        if shift and c == 0:
            pl.when(plane != donor)(start)
        elif shift and c == len(chunks) - 1:
            pl.when(plane != eager)(start)
        else:
            start()

    def to_helper(p):
        return pltpu.make_async_remote_copy(
            src_ref=rounded.at[:, pl.ds(sum(given[:p]), given[p]), :],
            dst_ref=moved_in.at[:, pl.ds(0, given[p]), :],
            send_sem=zsend,
            recv_sem=zrecv,
            device_id={"mp": p},
            device_id_type=MESH,
        )

    close = [o for o in order if o and far(o) < 2]
    distant = [o for o in order if far(o) >= 2]
    lead = 2 if shift else 1
    for turn, c in enumerate(turns):
        at = chunks[c]
        pltpu.make_async_copy(stage.at[:, at, :], stage.at[:, at, :], load_sem.at[c]).wait()
        for o in order:
            convert(o, at)
            if turn == 0 and o == order[0]:
                pl.semaphore_wait(barrier, entered)
                tell_chips(1)
                tell_below()
            if turn == 0 and o in close:
                gram_copy(o, c).start()
        if turn and turn < lead:
            send(c, close)
        elif turn >= lead:
            send(c, distant + close)
        if turn == lead - 1:
            for distance in range(1, bits):
                hear_chips(distance)
                tell_chips(distance + 1)
            for late in turns[:lead]:
                send(late, distant)
        if shift and c == 0:

            @pl.when(plane == donor)
            def _():
                for p in range(len(given)):
                    to_helper(p).start()
    if shift:

        @pl.when(plane == donor)
        def _():
            for o in close + distant:
                gram_copy(o, 0).start()

    for ox in range(chips):
        swap(ox).start()

    to_peer(1, rest_in, rest_in, osend, orecv).wait_recv()
    for ox in reversed(range(chips)):
        combine(ox)

    def relay_piece(p):
        for ox in rest_order:
            relay_copy(ox, p).start()

    def own_halves():
        for p in range(PIECES):
            for ox in rest_order:
                rest_copy(ox, ox - 1, p).start()

    def pass_on(p):
        for ox in rest_order:
            relay_copy(ox, p).wait_recv()
            at = pl.ds(p * piece, piece)
            there = flip(chip, 3 - ox, chips)
            add_to_rest(there, pl.ds((ox - 1) * half + p * piece, piece), relay[ox - 1, at, :])
            rest_copy(3 - ox, ox - 1, p).start()

    if shift:

        @pl.when(plane == eager)
        def _():
            relay_piece(0)
            for o in close + distant:
                gram_copy(o, len(chunks) - 1).start()

    pairs = [(i, k) for i in range(workers) for k in range(i, workers)]

    def gram(ref, at, accs, active=None):
        def one(step, accs):
            part_at = pl.ds(pl.multiple_of(at.start + step * TILE, TILE), TILE)
            xs = [ref[i, part_at, :].astype(jnp.float32) for i in range(workers)]
            lo = [x[:8] for x in xs]
            hi = [x[8:] for x in xs]
            return tuple(
                a + (lo[i] * lo[k] + hi[i] * hi[k]) for a, (i, k) in zip(accs, pairs)
            )

        steps = at.size // TILE
        if active is not None:
            steps = steps * active.astype(jnp.int32)
        return lax.fori_loop(0, steps, one, accs)

    def forward(o, p):
        at = pl.ds(0, given[p])
        return to_peer(o, moved_in.at[o, at, :], extra.at[me, at, :], fsend, frecv)

    def forwarded(p):
        whole = extra.at[pl.ds(0, workers - 1), pl.ds(0, given[p]), :]
        return to_peer(1, whole, whole, fsend, frecv)

    accs = tuple(jnp.zeros((8, LANES), jnp.float32) for _ in pairs)
    for c, at in enumerate(chunks):
        if shift and c == len(chunks) - 2:

            for p in range(len(given)):

                @pl.when(plane == p)
                def _(p=p):
                    to_helper(p).wait_recv()
                    for o in close + distant:
                        forward(o, p).start()
                    at = pl.ds(0, given[p])
                    extra[me, at, :] = moved_in[0, at, :]

        if split and c == len(chunks) - 1:
            if shift:
                pl.when(plane != eager)(lambda: relay_piece(0))
            else:
                relay_piece(0)
            for p in range(1, PIECES):
                relay_piece(p)
            own_halves()
            if shift:
                pl.when(plane == eager)(lambda: pass_on(0))
        if shift and c == 0:
          pl.when(plane != donor)(gram_chunk(c).wait_recv)
          accs = gram(recv, at, accs, plane != donor)
        else:
          gram_chunk(c).wait_recv()
          accs = gram(recv, at, accs)
        if c == 0:

            @pl.when(plane < planes - 1)
            def _():
                pl.semaphore_wait(risen, planes - 1 - plane)

            for o in range(1, workers):
                pl.semaphore_signal(
                    lines, inc=1, device_id={"worker": peer[o]}, device_id_type=MESH
                )
    if shift:
      for p in range(len(given)):
          pl.when(plane == p)(forwarded(p).wait_recv)
          accs = gram(extra, pl.ds(0, given[p]), accs, plane == p)

    value = dict(zip(pairs, accs))
    for i, k in pairs:
        if i == k:
            dist[i * workers + i] = jnp.zeros((8, LANES), jnp.float32)
        else:
            d = value[i, i] + value[k, k] - 2.0 * value[i, k]
            dist[i * workers + k] = d
            dist[k * workers + i] = d
    lists.wait()
    for i in range(workers):
        s = dist[i * workers + nb_ref[0, i]]
        for j in range(1, nb_ref.shape[0]):
            s = s + dist[i * workers + nb_ref[j, i]]
        part[pl.ds(i, 1), :] = jnp.sum(s, axis=0, keepdims=True)
    column = jnp.sum(part[...], axis=1, keepdims=True)
    line = lax.broadcasted_iota(jnp.int32, (workers, LANES), 0)
    lane = lax.broadcasted_iota(jnp.int32, (workers, LANES), 1)
    mine = plane * workers + me
    score_rows[mine] = jnp.sum(jnp.where(line == lane, column, 0.0), axis=0, keepdims=True)

    def score_copy(o, to):
        return pltpu.make_async_remote_copy(
            src_ref=score_rows.at[mine],
            dst_ref=score_rows.at[mine],
            send_sem=ssend,
            recv_sem=srecv,
            device_id={"worker": peer[o], "mp": to},
            device_id_type=MESH,
        )

    def all_scores():
        others = score_rows.at[pl.ds(0, workers * planes - 1)]
        return pltpu.make_async_remote_copy(
            src_ref=others,
            dst_ref=others,
            send_sem=ssend,
            recv_sem=srecv,
            device_id={"worker": peer[1], "mp": plane},
            device_id_type=MESH,
        )

    pl.semaphore_wait(lines, workers - 1)
    for to in range(planes):
        for o in order[:-1]:
            score_copy(o, to).start()

        @pl.when(plane != to)
        def _(to=to):
            score_copy(0, to).start()

    if split:
        if shift:
            pl.when(plane != eager)(lambda: pass_on(0))
        else:
            pass_on(0)
        for p in range(1, PIECES):
            pass_on(p)
    else:
        for ox in rest_order:
            for n in range(2):
                for p in range(PIECES):
                    rest_copy(ox, n, p).start()

    arrived = rest_recv.at[pl.ds(0, len(rest_order))]
    to_peer(1, arrived, arrived, rsend, rrecv).wait_recv()

    if shift:
        pl.when(plane == donor)(gram_chunk(0).wait_recv)
    for at in chunks:
        low = rest_in[chip, at, :].astype(jnp.float32)
        for ox in rest_order:
            low = low + rest_recv[ox, at, :].astype(jnp.float32)
        out_ref[at, :] = recv[win_ref[0], at, :].astype(jnp.float32) + low

    all_scores().wait_recv()
    total = jnp.sum(score_rows[...], axis=0) / jnp.float32(total_entries)
    scores_ref[...] = total[:, :workers]

    all_scores().wait_send()
    to_peer(1, rest_in, rest_in, osend, orecv).wait_send()
    if split:
        to_peer(1, relay, relay, ysend, yrecv.at[0, 0]).wait_send()
    sent = rounded.at[pl.ds(0, workers - 1)]
    to_peer(1, sent, sent, gsend, grecv.at[0]).wait_send()
    if shift:

        @pl.when(plane == donor)
        def _():
            whole = rounded.at[:, moved, :]
            to_peer(1, whole, whole, zsend, zrecv).wait_send()

        for p in range(len(given)):
            pl.when(plane == p)(forwarded(p).wait_send)

    to_peer(1, arrived, arrived, rsend, rrecv).wait_send()


def emit(scores_ref, block_ref, scores_out, block_out, sems):
    copies = [
        pltpu.make_async_copy(block_ref, block_out, sems.at[0]),
        pltpu.make_async_copy(scores_ref, scores_out, sems.at[1]),
    ]
    for copy in copies:
        copy.start()
    for copy in copies:
        copy.wait()


def solution(mesh):
    workers = mesh.shape["worker"]
    planes = mesh.shape["mp"]
    chips = workers // 2

    def body(gradients, neighbours, winner):
        length = gradients.shape[1]
        rows = length // (LANES * workers)
        given = shares(rows, chips, planes)
        starts = cuts(rows, given)
        entries = neighbours.shape[1] * length * planes
        bf16, f32 = jnp.bfloat16, jnp.float32
        dma = pltpu.SemaphoreType.DMA
        scores, aggregate = pl.pallas_call(
            functools.partial(kernel, workers, planes, entries),
            out_shape=(
                pltpu.VMEM((1, workers), f32),
                pltpu.VMEM((rows, LANES), f32),
            ),
            in_specs=[
                pl.BlockSpec(memory_space=pltpu.HBM),
                pl.BlockSpec(memory_space=pltpu.SMEM),
                pl.BlockSpec(memory_space=pltpu.HBM),
            ],
            out_specs=(
                pl.BlockSpec(memory_space=pltpu.VMEM),
                pl.BlockSpec(memory_space=pltpu.VMEM),
            ),
            scratch_shapes=[
                pltpu.SMEM(neighbours.shape[::-1], jnp.int32),
                pltpu.VMEM((workers, rows, LANES), f32),
                pltpu.VMEM((workers, rows, LANES), bf16),
                pltpu.VMEM((workers, rows, LANES), bf16),
                pltpu.VMEM((2, chips, rows, LANES), bf16),
                pltpu.VMEM((chips, rows, LANES), bf16),
                pltpu.VMEM((chips, rows, LANES), bf16),
                pltpu.VMEM((2, rows // 2, LANES), bf16),
                pltpu.VMEM((workers * workers, 8, LANES), f32),
                pltpu.VMEM((workers, LANES), f32),
                pltpu.VMEM((workers * planes, 1, LANES), f32),
                pltpu.VMEM((workers, max(given + [TILE]), LANES), bf16),
                pltpu.VMEM((workers, max(given + [TILE]), LANES), bf16),
                dma,
                dma((len(starts) - 1,)),
                dma,
                dma((len(starts) - 1,)),
                dma,
                dma,
                dma,
                dma((2, PIECES)),
                dma,
                dma,
                dma,
                dma,
                dma,
                dma,
                dma,
                dma,
                pltpu.SemaphoreType.REGULAR,
                pltpu.SemaphoreType.REGULAR((max(chips.bit_length() - 2, 1),)),
                pltpu.SemaphoreType.REGULAR,
            ],
            compiler_params=pltpu.CompilerParams(
                collective_id=0, has_side_effects=True, vmem_limit_bytes=63_500_000
            ),
        )(neighbours.T, winner, gradients.reshape(length // LANES, LANES))
        scores, aggregate = pl.pallas_call(
            emit,
            out_shape=(
                jax.ShapeDtypeStruct(scores.shape, f32),
                jax.ShapeDtypeStruct(aggregate.shape, f32),
            ),
            in_specs=[pl.BlockSpec(memory_space=pltpu.VMEM)] * 2,
            out_specs=(pl.BlockSpec(memory_space=pl.ANY),) * 2,
            scratch_shapes=[dma((2,))],
            compiler_params=pltpu.CompilerParams(vmem_limit_bytes=8 * 1024 * 1024),
        )(scores, aggregate)
        return scores.reshape(workers), aggregate.reshape(rows * LANES)

    in_specs = (P("worker", "mp"), P(), P())
    out_specs = (P(), P(("mp", "worker")))
    return jax.shard_map(body, mesh=mesh, in_specs=in_specs, out_specs=out_specs, check_vma=False)
```

```python
import functools

import jax
import jax.numpy as jnp
from jax import lax
from jax.experimental import pallas as pl
from jax.experimental.pallas import tpu as pltpu
from jax.sharding import PartitionSpec as P

MESH = pl.DeviceIdType.MESH
LANES = 128
CHUNKS = 4
SHARES = (1, 2)
PARTS = 32
TILE = 16
PIECES = 2


def flip(index, offset, size):
    result, bit = 0, 1
    while bit < size:
        digit = (index // bit) % 2
        if (offset // bit) % 2:
            digit = 1 - digit
        result = result + digit * bit
        bit *= 2
    return result


def shares(rows, chips, planes):
    unit = rows // PARTS // TILE * TILE
    return [unit * n for n in SHARES] if chips == planes == 4 and unit else []


def cuts(rows, given):
    first = sum(given)
    ends = [first + (rows - first) * n // CHUNKS // TILE * TILE for n in range(1, CHUNKS + 1)]
    return ([0, first] if first else [0]) + ends


def kernel(
    workers,
    planes,
    total_entries,
    nb_hbm,
    win_ref,
    g_ref,
    scores_ref,
    out_ref,
    nb_ref,
    stage,
    rounded,
    recv,
    rest,
    rest_in,
    rest_recv,
    relay,
    dist,
    part,
    score_rows,
    moved_in,
    extra,
    small_sem,
    load_sem,
    sent_sem,
    grecv,
    orecv,
    yrecv,
    rrecv,
    ssend,
    srecv,
    zrecv,
    frecv,
    risen,
    chip_hello,
    lines,
):
    me = lax.axis_index("worker")
    plane = lax.axis_index("mp")
    core = me % 2
    chip = me // 2
    chips = workers // 2
    rows = stage.shape[1]
    split = chips == 4
    given = shares(rows, chips, planes)
    shift = bool(given)
    donor, eager = planes - 1, 0
    starts = cuts(rows, given)
    chunks = [pl.ds(a, b - a) for a, b in zip(starts, starts[1:])]
    moved = chunks[0]
    bits = max(chips.bit_length() - 1, 0)

    def far(o):
        return bin(o // 2).count("1")

    order = sorted(range(2, workers), key=lambda o: (far(o), o // 2, o % 2)) + [1, 0]
    near = [o for o in range(1, workers) if far(o) < 2]
    peer = [flip(me, o, workers) for o in range(workers)]

    barrier = pltpu.get_barrier_semaphore()
    for o in near:
        pl.semaphore_signal(barrier, inc=1, device_id={"worker": peer[o]}, device_id_type=MESH)
    for p in range(1, planes):

        @pl.when(plane < p)
        def _(p=p):
            pl.semaphore_signal(barrier, inc=1, device_id={"mp": p}, device_id_type=MESH)

    entered = len(near) + plane

    def tell_chips(distance):
        for b in range(bits - distance):
            pl.semaphore_signal(
                chip_hello.at[distance - 1],
                inc=1,
                device_id={"worker": peer[2 << b]},
                device_id_type=MESH,
            )

    def hear_chips(distance):
        if bits > distance:
            pl.semaphore_wait(chip_hello.at[distance - 1], bits - distance)

    def tell_below():
        for p in range(planes - 1):

            @pl.when(p < plane)
            def _(p=p):
                pl.semaphore_signal(risen, inc=1, device_id={"mp": p}, device_id_type=MESH)

    turns = [1, 0] + list(range(2, len(chunks))) if shift else list(range(len(chunks)))
    for c in turns:
        at = chunks[c]
        for o in order:
            first = pl.multiple_of(peer[o] * rows, rows) + at.start
            pltpu.make_async_copy(
                g_ref.at[pl.ds(first, at.size), :], stage.at[o, at, :], load_sem.at[min(c, len(chunks) - 2)]
            ).start()
    lists = pltpu.make_async_copy(nb_hbm, nb_ref, small_sem)
    lists.start()

    def to_peer(o, src, dst, send_sem, recv_sem):
        return pltpu.make_async_remote_copy(
            src_ref=src,
            dst_ref=dst,
            send_sem=send_sem,
            recv_sem=recv_sem,
            device_id={"worker": peer[o]},
            device_id_type=MESH,
        )

    def gram_copy(o, c):
        at = chunks[c]
        return to_peer(o, rounded.at[o, at, :], recv.at[me, at, :], sent_sem, grecv.at[c])

    def gram_chunk(c):
        whole = recv.at[pl.ds(0, workers - 1), chunks[c], :]
        return to_peer(1, whole, whole, sent_sem, grecv.at[c])

    keep = jnp.where(win_ref[0] == me, 1.0, 0.0).astype(jnp.float32)

    def convert(o, at):
        x = stage[o, at, :]
        hi = x.astype(jnp.bfloat16)
        if o == 0:
            recv[me, at, :] = hi
        if o or (shift and at is moved):
            rounded[o, at, :] = hi
        low = ((x - hi.astype(jnp.float32)) * keep).astype(jnp.bfloat16)
        rest[peer[o] % 2, peer[o] // 2, at, :] = low

    def swap(ox):
        there = flip(chip, ox, chips)
        return to_peer(1, rest.at[1 - core, there], rest_in.at[there], sent_sem, orecv)

    def add_to_rest(there, at, other):
        rest_in[there, at, :] = rest_in[there, at, :] + other

    def combine(ox):
        there = flip(chip, ox, chips)
        for at in chunks:
            add_to_rest(there, at, rest[core, there, at, :])

    half = rows // 2
    piece = half // PIECES

    def relay_copy(ox, p):
        at = pl.ds(p * piece, piece)
        return to_peer(
            2 * ox,
            rest_in.at[flip(chip, 3, chips), pl.ds((ox - 1) * half + p * piece, piece), :],
            relay.at[ox - 1, at, :],
            sent_sem,
            yrecv.at[p],
        )

    def rest_copy(ox, n, p):
        at = pl.ds(n * half + p * piece, piece)
        return to_peer(
            2 * ox,
            rest_in.at[flip(chip, ox, chips), at, :],
            rest_recv.at[ox, at, :],
            sent_sem,
            rrecv,
        )

    rest_order = sorted(range(1, chips), key=lambda ox: bin(ox).count("1"))
    if split:
        rest_order = [1, 2]

    def send(c, peers):
        def start():
            for o in peers:
                gram_copy(o, c).start()

        if shift and c == 0:
            pl.when(plane != donor)(start)
        elif shift and c == len(chunks) - 1:
            pl.when(plane != eager)(start)
        else:
            start()

    def to_helper(p):
        return pltpu.make_async_remote_copy(
            src_ref=rounded.at[:, pl.ds(sum(given[:p]), given[p]), :],
            dst_ref=moved_in.at[:, pl.ds(0, given[p]), :],
            send_sem=sent_sem,
            recv_sem=zrecv,
            device_id={"mp": p},
            device_id_type=MESH,
        )

    close = [o for o in order if o and far(o) < 2]
    distant = [o for o in order if far(o) >= 2]
    lead = 2 if shift else 1
    for turn, c in enumerate(turns):
        at = chunks[c]
        if c < len(chunks) - 1:
            end = rows if c == len(chunks) - 2 else starts[c + 1]
            loaded = stage.at[:, pl.ds(at.start, end - at.start), :]
            pltpu.make_async_copy(loaded, loaded, load_sem.at[c]).wait()
        for o in order:
            convert(o, at)
            if turn == 0 and o == order[0]:
                pl.semaphore_wait(barrier, entered)
                tell_chips(1)
                tell_below()
            if turn == 0 and o in close:
                gram_copy(o, c).start()
        if turn and turn < lead:
            send(c, close)
        elif turn >= lead:
            send(c, distant + close)
        if turn == lead - 1:
            for distance in range(1, bits):
                hear_chips(distance)
                tell_chips(distance + 1)
            for late in turns[:lead]:
                send(late, distant)
        if shift and c == 0:

            @pl.when(plane == donor)
            def _():
                for p in range(len(given)):
                    to_helper(p).start()
    if shift:

        @pl.when(plane == donor)
        def _():
            for o in close + distant:
                gram_copy(o, 0).start()

    for ox in range(chips):
        swap(ox).start()

    to_peer(1, rest_in, rest_in, sent_sem, orecv).wait_recv()
    for ox in reversed(range(chips)):
        combine(ox)

    def relay_piece(p):
        for ox in rest_order:
            relay_copy(ox, p).start()

    def own_halves():
        for p in range(PIECES):
            for ox in rest_order:
                rest_copy(ox, ox - 1, p).start()

    def pass_on(p):
        at = pl.ds(p * piece, piece)
        to_peer(1, relay.at[:, at, :], relay.at[:, at, :], sent_sem, yrecv.at[p]).wait_recv()
        for ox in rest_order:
            there = flip(chip, 3 - ox, chips)
            add_to_rest(there, pl.ds((ox - 1) * half + p * piece, piece), relay[ox - 1, at, :])
            rest_copy(3 - ox, ox - 1, p).start()

    if shift:

        @pl.when(plane == eager)
        def _():
            relay_piece(0)
            for o in close + distant:
                gram_copy(o, len(chunks) - 1).start()

    pairs = [(i, k) for i in range(workers) for k in range(i, workers)]

    def gram(ref, at, accs, active=None):
        def one(step, accs):
            part_at = pl.ds(pl.multiple_of(at.start + step * TILE, TILE), TILE)
            xs = [ref[i, part_at, :].astype(jnp.float32) for i in range(workers)]
            lo = [x[:8] for x in xs]
            hi = [x[8:] for x in xs]
            return tuple(
                a + (lo[i] * lo[k] + hi[i] * hi[k]) for a, (i, k) in zip(accs, pairs)
            )

        steps = at.size // TILE
        if active is not None:
            steps = steps * active.astype(jnp.int32)
        return lax.fori_loop(0, steps, one, accs)

    def forward(o, p):
        at = pl.ds(0, given[p])
        return to_peer(o, moved_in.at[o, at, :], extra.at[me, at, :], sent_sem, frecv)

    def forwarded(p):
        whole = extra.at[pl.ds(0, workers - 1), pl.ds(0, given[p]), :]
        return to_peer(1, whole, whole, sent_sem, frecv)

    accs = tuple(jnp.zeros((8, LANES), jnp.float32) for _ in pairs)
    for c, at in enumerate(chunks):
        if shift and c == len(chunks) - 2:

            for p in range(len(given)):

                @pl.when(plane == p)
                def _(p=p):
                    to_helper(p).wait_recv()
                    for o in close + distant:
                        forward(o, p).start()
                    at = pl.ds(0, given[p])
                    extra[me, at, :] = moved_in[0, at, :]

        if split and c == len(chunks) - 1:
            if shift:
                pl.when(plane != eager)(lambda: relay_piece(0))
            else:
                relay_piece(0)
            for p in range(1, PIECES):
                relay_piece(p)
            own_halves()
            if shift:
                pl.when(plane == eager)(lambda: pass_on(0))
        if shift and c == 0:
          pl.when(plane != donor)(gram_chunk(c).wait_recv)
          accs = gram(recv, at, accs, plane != donor)
        else:
          gram_chunk(c).wait_recv()
          accs = gram(recv, at, accs)
        if c == 0:

            @pl.when(plane < planes - 1)
            def _():
                pl.semaphore_wait(risen, planes - 1 - plane)

            for o in range(1, workers):
                pl.semaphore_signal(
                    lines, inc=1, device_id={"worker": peer[o]}, device_id_type=MESH
                )
    if shift:
      for p in range(len(given)):
          pl.when(plane == p)(forwarded(p).wait_recv)
          accs = gram(extra, pl.ds(0, given[p]), accs, plane == p)

    value = dict(zip(pairs, accs))
    for i, k in pairs:
        if i == k:
            dist[i * workers + i] = jnp.zeros((8, LANES), jnp.float32)
        else:
            d = value[i, i] + value[k, k] - 2.0 * value[i, k]
            dist[i * workers + k] = d
            dist[k * workers + i] = d
    lists.wait()
    for i in range(workers):
        s = dist[i * workers + nb_ref[0, i]]
        for j in range(1, nb_ref.shape[0]):
            s = s + dist[i * workers + nb_ref[j, i]]
        part[pl.ds(i, 1), :] = jnp.sum(s, axis=0, keepdims=True)
    column = jnp.sum(part[...], axis=1, keepdims=True)
    line = lax.broadcasted_iota(jnp.int32, (workers, LANES), 0)
    lane = lax.broadcasted_iota(jnp.int32, (workers, LANES), 1)
    mine = plane * workers + me
    score_rows[mine] = jnp.sum(jnp.where(line == lane, column, 0.0), axis=0, keepdims=True)

    def score_copy(o, to):
        return pltpu.make_async_remote_copy(
            src_ref=score_rows.at[mine],
            dst_ref=score_rows.at[mine],
            send_sem=ssend,
            recv_sem=srecv,
            device_id={"worker": peer[o], "mp": to},
            device_id_type=MESH,
        )

    def all_scores():
        others = score_rows.at[pl.ds(0, workers * planes - 1)]
        return pltpu.make_async_remote_copy(
            src_ref=others,
            dst_ref=others,
            send_sem=ssend,
            recv_sem=srecv,
            device_id={"worker": peer[1], "mp": plane},
            device_id_type=MESH,
        )

    pl.semaphore_wait(lines, workers - 1)
    for to in range(planes):
        for o in order[:-1]:
            score_copy(o, to).start()

        @pl.when(plane != to)
        def _(to=to):
            score_copy(0, to).start()

    if split:
        if shift:
            pl.when(plane != eager)(lambda: pass_on(0))
        else:
            pass_on(0)
        for p in range(1, PIECES):
            pass_on(p)
    else:
        for ox in rest_order:
            for n in range(2):
                for p in range(PIECES):
                    rest_copy(ox, n, p).start()

    arrived = rest_recv.at[pl.ds(0, len(rest_order))]
    to_peer(1, arrived, arrived, sent_sem, rrecv).wait_recv()

    if shift:
        pl.when(plane == donor)(gram_chunk(0).wait_recv)
    for at in chunks:
        low = rest_in[chip, at, :].astype(jnp.float32)
        for ox in rest_order:
            low = low + rest_recv[ox, at, :].astype(jnp.float32)
        out_ref[at, :] = recv[win_ref[0], at, :].astype(jnp.float32) + low

    all_scores().wait_recv()
    total = jnp.sum(score_rows[...], axis=0) / jnp.float32(total_entries)
    scores_ref[...] = total[:, :workers]

    all_scores().wait_send()
    to_peer(1, rest_in, rest_in, sent_sem, orecv).wait_send()
    if split:
        to_peer(1, relay, relay, sent_sem, yrecv.at[0]).wait_send()
    sent = rounded.at[pl.ds(0, workers - 1)]
    to_peer(1, sent, sent, sent_sem, grecv.at[0]).wait_send()
    if shift:

        @pl.when(plane == donor)
        def _():
            whole = rounded.at[:, moved, :]
            to_peer(1, whole, whole, sent_sem, zrecv).wait_send()

        for p in range(len(given)):
            pl.when(plane == p)(forwarded(p).wait_send)

    to_peer(1, arrived, arrived, sent_sem, rrecv).wait_send()


def emit(scores_ref, block_ref, scores_out, block_out, sems):
    copies = [
        pltpu.make_async_copy(block_ref, block_out, sems.at[0]),
        pltpu.make_async_copy(scores_ref, scores_out, sems.at[1]),
    ]
    for copy in copies:
        copy.start()
    for copy in copies:
        copy.wait()


def solution(mesh):
    workers = mesh.shape["worker"]
    planes = mesh.shape["mp"]
    chips = workers // 2

    def body(gradients, neighbours, winner):
        length = gradients.shape[1]
        rows = length // (LANES * workers)
        given = shares(rows, chips, planes)
        starts = cuts(rows, given)
        entries = neighbours.shape[1] * length * planes
        bf16, f32 = jnp.bfloat16, jnp.float32
        dma = pltpu.SemaphoreType.DMA
        scores, aggregate = pl.pallas_call(
            functools.partial(kernel, workers, planes, entries),
            out_shape=(
                pltpu.VMEM((1, workers), f32),
                pltpu.VMEM((rows, LANES), f32),
            ),
            in_specs=[
                pl.BlockSpec(memory_space=pltpu.HBM),
                pl.BlockSpec(memory_space=pltpu.SMEM),
                pl.BlockSpec(memory_space=pltpu.HBM),
            ],
            out_specs=(
                pl.BlockSpec(memory_space=pltpu.VMEM),
                pl.BlockSpec(memory_space=pltpu.VMEM),
            ),
            scratch_shapes=[
                pltpu.SMEM(neighbours.shape[::-1], jnp.int32),
                pltpu.VMEM((workers, rows, LANES), f32),
                pltpu.VMEM((workers, rows, LANES), bf16),
                pltpu.VMEM((workers, rows, LANES), bf16),
                pltpu.VMEM((2, chips, rows, LANES), bf16),
                pltpu.VMEM((chips, rows, LANES), bf16),
                pltpu.VMEM((chips, rows, LANES), bf16),
                pltpu.VMEM((2, rows // 2, LANES), bf16),
                pltpu.VMEM((workers * workers, 8, LANES), f32),
                pltpu.VMEM((workers, LANES), f32),
                pltpu.VMEM((workers * planes, 1, LANES), f32),
                pltpu.VMEM((workers, max(given + [TILE]), LANES), bf16),
                pltpu.VMEM((workers, max(given + [TILE]), LANES), bf16),
                dma,
                dma((len(starts) - 2,)),
                dma,
                dma((len(starts) - 1,)),
                dma,
                dma((PIECES,)),
                dma,
                dma,
                dma,
                dma,
                dma,
                pltpu.SemaphoreType.REGULAR,
                pltpu.SemaphoreType.REGULAR((max(chips.bit_length() - 2, 1),)),
                pltpu.SemaphoreType.REGULAR,
            ],
            compiler_params=pltpu.CompilerParams(
                collective_id=0, has_side_effects=True, vmem_limit_bytes=63_500_000
            ),
        )(neighbours.T, winner, gradients.reshape(length // LANES, LANES))
        scores, aggregate = pl.pallas_call(
            emit,
            out_shape=(
                jax.ShapeDtypeStruct(scores.shape, f32),
                jax.ShapeDtypeStruct(aggregate.shape, f32),
            ),
            in_specs=[pl.BlockSpec(memory_space=pltpu.VMEM)] * 2,
            out_specs=(pl.BlockSpec(memory_space=pl.ANY),) * 2,
            scratch_shapes=[dma((2,))],
            compiler_params=pltpu.CompilerParams(vmem_limit_bytes=8 * 1024 * 1024),
        )(scores, aggregate)
        return scores.reshape(workers), aggregate.reshape(rows * LANES)

    in_specs = (P("worker", "mp"), P(), P())
    out_specs = (P(), P(("mp", "worker")))
    return jax.shard_map(body, mesh=mesh, in_specs=in_specs, out_specs=out_specs, check_vma=False)
```

```python
import functools

import jax
import jax.numpy as jnp
from jax import lax
from jax.experimental import pallas as pl
from jax.experimental.pallas import tpu as pltpu
from jax.sharding import PartitionSpec as P

MESH = pl.DeviceIdType.MESH
LANES = 128
CHUNKS = 4
SHARES = (1, 2)
PARTS = 32
TILE = 16
PIECES = 2


def flip(index, offset, size):
    result, bit = 0, 1
    while bit < size:
        digit = (index // bit) % 2
        if (offset // bit) % 2:
            digit = 1 - digit
        result = result + digit * bit
        bit *= 2
    return result


def shares(rows, chips, planes):
    unit = rows // PARTS // TILE * TILE
    return [unit * n for n in SHARES] if chips == planes == 4 and unit else []


def cuts(rows, given):
    first = sum(given)
    ends = [first + (rows - first) * n // CHUNKS // TILE * TILE for n in range(1, CHUNKS + 1)]
    return ([0, first] if first else [0]) + ends


def kernel(
    workers,
    planes,
    total_entries,
    nb_hbm,
    win_ref,
    g_ref,
    scores_ref,
    out_ref,
    nb_ref,
    stage,
    rounded,
    recv,
    rest,
    rest_in,
    rest_recv,
    relay,
    dist,
    part,
    score_rows,
    moved_in,
    extra,
    small_sem,
    load_sem,
    sent_sem,
    grecv,
    orecv,
    yrecv,
    rrecv,
    ssend,
    srecv,
    zrecv,
    frecv,
    risen,
    chip_hello,
    lines,
):
    me = lax.axis_index("worker")
    plane = lax.axis_index("mp")
    core = me % 2
    chip = me // 2
    chips = workers // 2
    rows = stage.shape[1]
    split = chips == 4
    given = shares(rows, chips, planes)
    shift = bool(given)
    donor, eager = planes - 1, 0
    starts = cuts(rows, given)
    chunks = [pl.ds(a, b - a) for a, b in zip(starts, starts[1:])]
    moved = chunks[0]
    bits = max(chips.bit_length() - 1, 0)

    def far(o):
        return bin(o // 2).count("1")

    order = sorted(range(2, workers), key=lambda o: (far(o), o // 2, o % 2)) + [1, 0]
    near = [o for o in range(1, workers) if far(o) < 2]
    peer = [flip(me, o, workers) for o in range(workers)]

    barrier = pltpu.get_barrier_semaphore()
    for o in near:
        pl.semaphore_signal(barrier, inc=1, device_id={"worker": peer[o]}, device_id_type=MESH)
    for p in range(1, planes):

        @pl.when(plane < p)
        def _(p=p):
            pl.semaphore_signal(barrier, inc=1, device_id={"mp": p}, device_id_type=MESH)

    entered = len(near) + plane

    def tell_chips(distance):
        for b in range(bits - distance):
            pl.semaphore_signal(
                chip_hello.at[distance - 1],
                inc=1,
                device_id={"worker": peer[2 << b]},
                device_id_type=MESH,
            )

    def hear_chips(distance):
        if bits > distance:
            pl.semaphore_wait(chip_hello.at[distance - 1], bits - distance)

    def tell_below():
        for p in range(planes - 1):

            @pl.when(p < plane)
            def _(p=p):
                pl.semaphore_signal(risen, inc=1, device_id={"mp": p}, device_id_type=MESH)

    turns = [1, 0] + list(range(2, len(chunks))) if shift else list(range(len(chunks)))
    for c in turns:
        at = chunks[c]
        for o in order:
            first = pl.multiple_of(peer[o] * rows, rows) + at.start
            pltpu.make_async_copy(
                g_ref.at[pl.ds(first, at.size), :], stage.at[o, at, :], load_sem.at[min(c, len(chunks) - 2)]
            ).start()
    lists = pltpu.make_async_copy(nb_hbm, nb_ref, small_sem)
    lists.start()

    def to_peer(o, src, dst, send_sem, recv_sem):
        return pltpu.make_async_remote_copy(
            src_ref=src,
            dst_ref=dst,
            send_sem=send_sem,
            recv_sem=recv_sem,
            device_id={"worker": peer[o]},
            device_id_type=MESH,
        )

    def gram_copy(o, c):
        at = chunks[c]
        return to_peer(o, rounded.at[o, at, :], recv.at[me, at, :], sent_sem, grecv.at[c])

    def gram_chunk(c):
        whole = recv.at[pl.ds(0, workers - 1), chunks[c], :]
        return to_peer(1, whole, whole, sent_sem, grecv.at[c])

    keep = jnp.where(win_ref[0] == me, 1.0, 0.0).astype(jnp.float32)

    def convert(o, at):
        x = stage[o, at, :]
        hi = x.astype(jnp.bfloat16)
        if o == 0:
            recv[me, at, :] = hi
        if o or (shift and at is moved):
            rounded[o, at, :] = hi
        low = ((x - hi.astype(jnp.float32)) * keep).astype(jnp.bfloat16)
        rest[peer[o] % 2, peer[o] // 2, at, :] = low

    def swap(ox):
        there = flip(chip, ox, chips)
        return to_peer(1, rest.at[1 - core, there], rest_in.at[there], sent_sem, orecv)

    def add_to_rest(there, at, other):
        rest_in[there, at, :] = rest_in[there, at, :] + other

    def combine(ox):
        there = flip(chip, ox, chips)
        for at in chunks:
            add_to_rest(there, at, rest[core, there, at, :])

    half = rows // 2
    piece = half // PIECES

    def relay_copy(ox, p):
        at = pl.ds(p * piece, piece)
        return to_peer(
            2 * ox,
            rest_in.at[flip(chip, 3, chips), pl.ds((ox - 1) * half + p * piece, piece), :],
            relay.at[ox - 1, at, :],
            sent_sem,
            yrecv.at[p],
        )

    def rest_copy(ox, n, p):
        at = pl.ds(n * half + p * piece, piece)
        return to_peer(
            2 * ox,
            rest_in.at[flip(chip, ox, chips), at, :],
            rest_recv.at[ox, at, :],
            sent_sem,
            rrecv,
        )

    rest_order = sorted(range(1, chips), key=lambda ox: bin(ox).count("1"))
    if split:
        rest_order = [1, 2]

    def send(c, peers):
        def start():
            for o in peers:
                gram_copy(o, c).start()

        if shift and c == 0:
            pl.when(plane != donor)(start)
        elif shift and c == len(chunks) - 1:
            pl.when(plane != eager)(start)
        else:
            start()

    def to_helper(p):
        return pltpu.make_async_remote_copy(
            src_ref=rounded.at[:, pl.ds(sum(given[:p]), given[p]), :],
            dst_ref=moved_in.at[:, pl.ds(0, given[p]), :],
            send_sem=sent_sem,
            recv_sem=zrecv,
            device_id={"mp": p},
            device_id_type=MESH,
        )

    close = [o for o in order if o and far(o) < 2]
    distant = [o for o in order if far(o) >= 2]
    lead = 2 if shift else 1
    for turn, c in enumerate(turns):
        at = chunks[c]
        if c < len(chunks) - 1:
            end = rows if c == len(chunks) - 2 else starts[c + 1]
            loaded = stage.at[:, pl.ds(at.start, end - at.start), :]
            pltpu.make_async_copy(loaded, loaded, load_sem.at[c]).wait()
        for o in order:
            convert(o, at)
            if turn == 0 and o == order[0]:
                pl.semaphore_wait(barrier, entered)
                tell_chips(1)
                tell_below()
            if turn == 0 and o in close:
                gram_copy(o, c).start()
        if turn and turn < lead:
            send(c, close)
        elif turn >= lead:
            send(c, distant + close)
        if turn == lead - 1:
            for distance in range(1, bits):
                hear_chips(distance)
                tell_chips(distance + 1)
            for late in turns[:lead]:
                send(late, distant)
        if shift and c == 0:

            @pl.when(plane == donor)
            def _():
                for p in range(len(given)):
                    to_helper(p).start()
    if shift:

        @pl.when(plane == donor)
        def _():
            for o in close + distant:
                gram_copy(o, 0).start()

    for ox in range(chips):
        swap(ox).start()

    to_peer(1, rest_in, rest_in, sent_sem, orecv).wait_recv()
    for ox in reversed(range(chips)):
        combine(ox)

    def relay_piece(p):
        for ox in rest_order:
            relay_copy(ox, p).start()

    def own_halves():
        for p in range(PIECES):
            for ox in rest_order:
                rest_copy(ox, ox - 1, p).start()

    def pass_on(p):
        at = pl.ds(p * piece, piece)
        to_peer(1, relay.at[:, at, :], relay.at[:, at, :], sent_sem, yrecv.at[p]).wait_recv()
        for ox in rest_order:
            there = flip(chip, 3 - ox, chips)
            add_to_rest(there, pl.ds((ox - 1) * half + p * piece, piece), relay[ox - 1, at, :])
            rest_copy(3 - ox, ox - 1, p).start()

    if shift:

        @pl.when(plane == eager)
        def _():
            relay_piece(0)
            for o in close + distant:
                gram_copy(o, len(chunks) - 1).start()

    pairs = [(i, k) for i in range(workers) for k in range(i, workers)]

    def gram(ref, at, accs, active=None):
        def one(step, accs):
            part_at = pl.ds(pl.multiple_of(at.start + step * TILE, TILE), TILE)
            xs = [ref[i, part_at, :].astype(jnp.float32) for i in range(workers)]
            lo = [x[:8] for x in xs]
            hi = [x[8:] for x in xs]
            return tuple(
                a + (lo[i] * lo[k] + hi[i] * hi[k]) for a, (i, k) in zip(accs, pairs)
            )

        steps = at.size // TILE
        if active is not None:
            steps = steps * active.astype(jnp.int32)
        return lax.fori_loop(0, steps, one, accs)

    def forward(o, p):
        at = pl.ds(0, given[p])
        return to_peer(o, moved_in.at[o, at, :], extra.at[me, at, :], sent_sem, frecv)

    def forwarded(p):
        whole = extra.at[pl.ds(0, workers - 1), pl.ds(0, given[p]), :]
        return to_peer(1, whole, whole, sent_sem, frecv)

    accs = tuple(jnp.zeros((8, LANES), jnp.float32) for _ in pairs)
    for c, at in enumerate(chunks):
        if shift and c == len(chunks) - 2:

            for p in range(len(given)):

                @pl.when(plane == p)
                def _(p=p):
                    to_helper(p).wait_recv()
                    for o in close + distant:
                        forward(o, p).start()
                    at = pl.ds(0, given[p])
                    extra[me, at, :] = moved_in[0, at, :]

        if split and c == len(chunks) - 1:
            if shift:
                pl.when(plane != eager)(lambda: relay_piece(0))
            else:
                relay_piece(0)
            for p in range(1, PIECES):
                relay_piece(p)
            own_halves()
            if shift:
                pl.when(plane == eager)(lambda: pass_on(0))
        if shift and c == 0:
          pl.when(plane != donor)(gram_chunk(c).wait_recv)
          accs = gram(recv, at, accs, plane != donor)
        else:
          gram_chunk(c).wait_recv()
          accs = gram(recv, at, accs)
        if c == 0:

            @pl.when(plane < planes - 1)
            def _():
                pl.semaphore_wait(risen, planes - 1 - plane)

            for o in range(1, workers):
                pl.semaphore_signal(
                    lines, inc=1, device_id={"worker": peer[o]}, device_id_type=MESH
                )
    if shift:
      for p in range(len(given)):
          pl.when(plane == p)(forwarded(p).wait_recv)
          accs = gram(extra, pl.ds(0, given[p]), accs, plane == p)

    value = dict(zip(pairs, accs))
    for i, k in pairs:
        if i < k:
            d = value[i, i] + value[k, k] - 2.0 * value[i, k]
            dist[i * workers + k] = d
            dist[k * workers + i] = d
    lists.wait()
    for i in range(workers):
        s = dist[i * workers + nb_ref[0, i]]
        for j in range(1, nb_ref.shape[0]):
            s = s + dist[i * workers + nb_ref[j, i]]
        part[pl.ds(i, 1), :] = jnp.sum(s, axis=0, keepdims=True)
    column = jnp.sum(part[...], axis=1, keepdims=True)
    line = lax.broadcasted_iota(jnp.int32, (workers, LANES), 0)
    lane = lax.broadcasted_iota(jnp.int32, (workers, LANES), 1)
    mine = plane * workers + me
    score_rows[mine] = jnp.sum(jnp.where(line == lane, column, 0.0), axis=0, keepdims=True)

    def score_copy(o, to):
        return pltpu.make_async_remote_copy(
            src_ref=score_rows.at[mine],
            dst_ref=score_rows.at[mine],
            send_sem=ssend,
            recv_sem=srecv,
            device_id={"worker": peer[o], "mp": to},
            device_id_type=MESH,
        )

    def all_scores():
        others = score_rows.at[pl.ds(0, workers * planes - 1)]
        return pltpu.make_async_remote_copy(
            src_ref=others,
            dst_ref=others,
            send_sem=ssend,
            recv_sem=srecv,
            device_id={"worker": peer[1], "mp": plane},
            device_id_type=MESH,
        )

    pl.semaphore_wait(lines, workers - 1)
    for to in range(planes):
        for o in distant + close:
            score_copy(o, to).start()

        @pl.when(plane != to)
        def _(to=to):
            score_copy(0, to).start()

    if split:
        if shift:
            pl.when(plane != eager)(lambda: pass_on(0))
        else:
            pass_on(0)
        for p in range(1, PIECES):
            pass_on(p)
    else:
        for ox in rest_order:
            for n in range(2):
                for p in range(PIECES):
                    rest_copy(ox, n, p).start()

    arrived = rest_recv.at[pl.ds(0, len(rest_order))]
    to_peer(1, arrived, arrived, sent_sem, rrecv).wait_recv()

    if shift:
        pl.when(plane == donor)(gram_chunk(0).wait_recv)
    for at in chunks:
        low = rest_in[chip, at, :].astype(jnp.float32)
        for ox in rest_order:
            low = low + rest_recv[ox, at, :].astype(jnp.float32)
        out_ref[at, :] = recv[win_ref[0], at, :].astype(jnp.float32) + low

    all_scores().wait_recv()
    total = jnp.sum(score_rows[...], axis=0) / jnp.float32(total_entries)
    scores_ref[...] = total[:, :workers]

    all_scores().wait_send()
    to_peer(1, rest_in, rest_in, sent_sem, orecv).wait_send()
    if split:
        to_peer(1, relay, relay, sent_sem, yrecv.at[0]).wait_send()
    sent = rounded.at[pl.ds(0, workers - 1)]
    to_peer(1, sent, sent, sent_sem, grecv.at[0]).wait_send()
    if shift:

        @pl.when(plane == donor)
        def _():
            whole = rounded.at[:, moved, :]
            to_peer(1, whole, whole, sent_sem, zrecv).wait_send()

        for p in range(len(given)):
            pl.when(plane == p)(forwarded(p).wait_send)

    to_peer(1, arrived, arrived, sent_sem, rrecv).wait_send()


def emit(scores_ref, block_ref, scores_out, block_out, sems):
    copies = [
        pltpu.make_async_copy(block_ref, block_out, sems.at[0]),
        pltpu.make_async_copy(scores_ref, scores_out, sems.at[1]),
    ]
    for copy in copies:
        copy.start()
    for copy in copies:
        copy.wait()


def solution(mesh):
    workers = mesh.shape["worker"]
    planes = mesh.shape["mp"]
    chips = workers // 2

    def body(gradients, neighbours, winner):
        length = gradients.shape[1]
        rows = length // (LANES * workers)
        given = shares(rows, chips, planes)
        starts = cuts(rows, given)
        entries = neighbours.shape[1] * length * planes
        bf16, f32 = jnp.bfloat16, jnp.float32
        dma = pltpu.SemaphoreType.DMA
        scores, aggregate = pl.pallas_call(
            functools.partial(kernel, workers, planes, entries),
            out_shape=(
                pltpu.VMEM((1, workers), f32),
                pltpu.VMEM((rows, LANES), f32),
            ),
            in_specs=[
                pl.BlockSpec(memory_space=pltpu.HBM),
                pl.BlockSpec(memory_space=pltpu.SMEM),
                pl.BlockSpec(memory_space=pltpu.HBM),
            ],
            out_specs=(
                pl.BlockSpec(memory_space=pltpu.VMEM),
                pl.BlockSpec(memory_space=pltpu.VMEM),
            ),
            scratch_shapes=[
                pltpu.SMEM(neighbours.shape[::-1], jnp.int32),
                pltpu.VMEM((workers, rows, LANES), f32),
                pltpu.VMEM((workers, rows, LANES), bf16),
                pltpu.VMEM((workers, rows, LANES), bf16),
                pltpu.VMEM((2, chips, rows, LANES), bf16),
                pltpu.VMEM((chips, rows, LANES), bf16),
                pltpu.VMEM((chips, rows, LANES), bf16),
                pltpu.VMEM((2, rows // 2, LANES), bf16),
                pltpu.VMEM((workers * workers, 8, LANES), f32),
                pltpu.VMEM((workers, LANES), f32),
                pltpu.VMEM((workers * planes, 1, LANES), f32),
                pltpu.VMEM((workers, max(given + [TILE]), LANES), bf16),
                pltpu.VMEM((workers, max(given + [TILE]), LANES), bf16),
                dma,
                dma((len(starts) - 2,)),
                dma,
                dma((len(starts) - 1,)),
                dma,
                dma((PIECES,)),
                dma,
                dma,
                dma,
                dma,
                dma,
                pltpu.SemaphoreType.REGULAR,
                pltpu.SemaphoreType.REGULAR((max(chips.bit_length() - 2, 1),)),
                pltpu.SemaphoreType.REGULAR,
            ],
            compiler_params=pltpu.CompilerParams(
                collective_id=0, has_side_effects=True, vmem_limit_bytes=63_500_000
            ),
        )(neighbours.T, winner, gradients.reshape(length // LANES, LANES))
        scores, aggregate = pl.pallas_call(
            emit,
            out_shape=(
                jax.ShapeDtypeStruct(scores.shape, f32),
                jax.ShapeDtypeStruct(aggregate.shape, f32),
            ),
            in_specs=[pl.BlockSpec(memory_space=pltpu.VMEM)] * 2,
            out_specs=(pl.BlockSpec(memory_space=pl.ANY),) * 2,
            scratch_shapes=[dma((2,))],
            compiler_params=pltpu.CompilerParams(vmem_limit_bytes=8 * 1024 * 1024),
        )(scores, aggregate)
        return scores.reshape(workers), aggregate.reshape(rows * LANES)

    in_specs = (P("worker", "mp"), P(), P())
    out_specs = (P(), P(("mp", "worker")))
    return jax.shard_map(body, mesh=mesh, in_specs=in_specs, out_specs=out_specs, check_vma=False)
```
